32 devices in a mesh: elem: 8 (over z, y), chan: 4 (over x, core).
Axes of the slice: x: 2, y: 2, z: 4, core: 2. Of those that a mesh axis runs over, the one named last changes fastest.
Arguments:
- voltages: bfloat16 [2, 1024, 19584], P(None, ('elem', 'chan')), may hold values from -6 to 6
- delays: int32 [1024], P(('elem', 'chan')), may hold values from 0 to 127
- prototype: bfloat16 [16, 1024], replicated, may hold values from -1.5 to 1.5
- subband_map: int32 [16], replicated, may hold values from 0 to 1023, as said below
- beam_weights: bfloat16 [512, 2, 16, 1024], P('elem', None, 'chan'), may hold values from -0.25 to 0.25
Outputs:
- element_power: bfloat16 [1024, 1024], P(('elem', 'chan'))
- beam_voltages: float32 [2, 64, 512], P(None, 'chan', 'elem')
The draws below stay inside these ranges and needn't reach their ends.
Inputs may be any that keep to these rules, and one draw needn't show every extreme that they name: `subband_map`: distinct channel numbers.
All inputs are finite; a program needn't handle non-finite values.
Results may differ from the reference program's by a relative error of at most 0.007.
Values may be sent and summed in bfloat16 or wider, within the bound.
A program may use at most 128 MiB of HBM per device.

```python
import math
import jax
import jax.numpy as jnp
from jax import lax

CH = 1024
TAPS = 16
BEAMS = 512
E_DEV = 32
FRAMES = 4
MAXD = 128
ELEMS = 1024
SUB = 16
SAMP = 19584


def draw_subband_map(key, part):
    return jax.random.permutation(key, CH)[:SUB].astype(jnp.int32)


def plant(values, rng, smallest, top_value):
    extent = values.shape
    index_at = [jax.random.randint(jax.random.fold_in(rng, axis), (), 0, extent[axis]) for axis in range(len(extent))]
    values = values.at[tuple(index_at)].set(smallest)
    longest = extent.index(max(extent))
    index_at[longest] = (index_at[longest] + 1) % extent[longest]
    return values.at[tuple(index_at)].set(top_value)


def with_spikes(result, key, source, target, parts, factor):
    def block_of(position):
        return (jnp.arange(result.shape[position]) // (result.shape[position] // parts)).reshape((-1,) + (1,) * (result.ndim - 1 - position))

    near = jax.random.permutation(key, parts)[block_of(target)]
    other_side = (block_of(target) + parts // 2) % parts
    return jnp.where((block_of(source) == near) | (block_of(source) == other_side), factor * result, result)


def block_levels(key, extent, split, least, high):
    def one(axis_at, blocks):
        draws = jax.random.uniform(jax.random.fold_in(jax.random.fold_in(key, 6), axis_at), (blocks,), jnp.float32, least / len(split), high / len(split))
        return jnp.repeat(jnp.exp(draws), extent[axis_at] // blocks).reshape((-1,) + (1,) * (len(extent) - axis_at - 1))

    gain = one(*split[0])
    for cut in split[1:]:
        gain = gain * one(*cut)
    return gain


def normal_values(stream_key, extent, scale, limit, shards=(), held_as=jnp.bfloat16):
    entries = scale * jax.random.normal(stream_key, extent, jnp.float32)
    if shards:
        entries = entries * block_levels(stream_key, extent, shards, -0.22, 0.18)
    return jnp.clip(entries, -limit, limit).astype(held_as)


def bell_draw_with(own_key, dims, spread, bound, split, heavy, kind=jnp.bfloat16):
    drawn = spread * jax.random.normal(own_key, dims, jnp.float32)
    if split:
        drawn = drawn * block_levels(own_key, dims, split, -0.22, 0.18)
    return jnp.clip(with_spikes(drawn, jax.random.fold_in(own_key, 3), *heavy), -bound, bound).astype(kind)


def setup_inputs(seed: int = 0) -> dict:
    seeds = jax.random.split(jax.random.key(seed), 6)
    voltages = normal_values(seeds[0], (2, ELEMS, SAMP), 1.0, 6.0, ((1, 32),))
    delays = plant(jax.random.randint(seeds[1], (ELEMS,), 0, MAXD), jax.random.fold_in(seeds[1], 1), 0, MAXD - 1).astype(jnp.int32)
    prototype = normal_values(seeds[2], (TAPS, CH), 0.25, 1.5)
    subband_map = draw_subband_map(jax.random.fold_in(seeds[5], 71), 0)
    beam_weights = bell_draw_with(seeds[4], (BEAMS, 2, SUB, ELEMS), ELEMS ** -0.5, 0.25, ((0, 8), (2, 4)), (3, 0, 8, 2.0))
    return {"voltages": voltages, "delays": delays, "prototype": prototype, "subband_map": subband_map, "beam_weights": beam_weights}


def filtered(voltages, delays, prototype):
    tap_count, chan_count = prototype.shape
    blocks = FRAMES + tap_count - 1
    window_len = blocks * chan_count

    def window(samples, offset):
        return lax.dynamic_slice_in_dim(samples, offset, window_len, 0)
    segments = jax.vmap(jax.vmap(window, in_axes=(0, 0)), in_axes=(0, None))(voltages, delays.astype(jnp.int32))
    segments = segments.reshape(voltages.shape[0], voltages.shape[1], blocks, chan_count)
    coeffs = prototype.astype(jnp.float32)
    running = jnp.zeros((voltages.shape[0], voltages.shape[1], FRAMES, chan_count), jnp.float32)
    for tap_index in range(tap_count):
        running = running + coeffs[tap_index] * segments[:, :, tap_index:tap_index + FRAMES, :].astype(jnp.float32)
    return running.astype(jnp.bfloat16)

def reference(voltages, delays, prototype, subband_map, beam_weights):
    groups = ELEMS // E_DEV

    def one_group(number):
        first_elem = number * E_DEV
        voltage_block = lax.dynamic_slice_in_dim(voltages, first_elem, E_DEV, 1)
        shifts = lax.dynamic_slice_in_dim(delays, first_elem, E_DEV, 0)
        filtered_wave = filtered(voltage_block, shifts, prototype)
        signal = filtered_wave[0].astype(jnp.float32) + 1j * filtered_wave[1].astype(jnp.float32)
        spectrum = jnp.fft.fft(signal, axis=-1) / math.sqrt(CH)
        spec_real = jnp.real(spectrum)
        spec_imag = jnp.imag(spectrum)
        power_block = lax.optimization_barrier(jnp.mean(spec_real * spec_real + spec_imag * spec_imag, axis=1)).astype(jnp.bfloat16)
        chosen = jnp.stack([spec_real[:, :, subband_map], spec_imag[:, :, subband_map]]).astype(jnp.bfloat16)
        return (power_block, chosen)
    power_all, chosen_groups = lax.map(one_group, jnp.arange(groups, dtype=jnp.int32))
    element_power = power_all.reshape(ELEMS, CH)
    chosen_all = jnp.transpose(chosen_groups, (1, 4, 3, 0, 2)).reshape(2, SUB, FRAMES, ELEMS)

    def one_subband(number):
        weight_slice = lax.dynamic_index_in_dim(beam_weights, number, 2, keepdims=False)
        spec_slice = lax.dynamic_index_in_dim(chosen_all, number, 1, keepdims=False)

        def contract(spectral, weighting):
            return jnp.dot(spectral, weighting.T, preferred_element_type=jnp.float32)
        out_real = contract(spec_slice[0], weight_slice[:, 0]) - contract(spec_slice[1], weight_slice[:, 1])
        out_imag = contract(spec_slice[1], weight_slice[:, 0]) + contract(spec_slice[0], weight_slice[:, 1])
        return jnp.stack([out_real, out_imag])
    stacked = lax.map(one_subband, jnp.arange(SUB, dtype=jnp.int32))
    beam_voltages = jnp.transpose(stacked, (1, 0, 2, 3)).reshape(2, SUB * FRAMES, BEAMS)
    return (element_power, beam_voltages)
```

```python
import functools
import math

import jax
import jax.numpy as jnp
import numpy as np
from jax import lax
from jax.experimental import pallas as pl
from jax.experimental.pallas import tpu as pltpu
from jax.sharding import PartitionSpec as P

FRAMES = 4
LANES = 128
RADIX = 8
MESH = pl.DeviceIdType.MESH


def fir_kernel(delays_ref, volt_ref, proto_ref, out_ref, seg_ref, coef_ref):
    rows = volt_ref.shape[1]
    taps, chan = proto_ref.shape
    per = chan // LANES
    blocks = FRAMES + taps - 1
    columns = blocks * per
    part, group = pl.program_id(0), pl.program_id(1)

    @pl.when((part == 0) & (group == 0))
    def _():
        for t in range(taps):
            coef_ref[t] = jnp.broadcast_to(
                proto_ref[pl.ds(t, 1), :].astype(jnp.float32), (8, chan)
            )

    lane = lax.broadcasted_iota(jnp.int32, (8, LANES), 1)
    sub = lax.broadcasted_iota(jnp.int32, (8, LANES), 0)
    halves = rows // 8
    index, keep = [], []
    for h in range(halves):
        shift = jnp.zeros((8, LANES), jnp.int32)
        for i in range(8):
            shift = jnp.where(sub == i, delays_ref[group * rows + h * 8 + i], shift)
        index.append((lane + shift) % LANES)
        keep.append(lane < LANES - shift)

    def turned(c):
        both = volt_ref[0, :, pl.ds(c * LANES, LANES)].astype(jnp.float32)
        return [
            jnp.take_along_axis(
                both[8 * h : 8 * h + 8], index[h], axis=1, mode="promise_in_bounds"
            )
            for h in range(halves)
        ]

    now = turned(0)
    for c in range(columns):
        nxt = turned(c + 1)
        for h in range(halves):
            seg_ref[h, :, pl.ds(c * LANES, LANES)] = jnp.where(keep[h], now[h], nxt[h])
        now = nxt
    for j in range(per):
        sums = [[None] * halves for _ in range(FRAMES)]
        for h in range(halves):
            held = [seg_ref[h, :, pl.ds((b * per + j) * LANES, LANES)] for b in range(blocks)]
            for t in range(taps):
                coef = coef_ref[t, :, pl.ds(j * LANES, LANES)]
                for f in range(FRAMES):
                    term = coef * held[f + t]
                    sums[f][h] = term if t == 0 else sums[f][h] + term
        for f in range(FRAMES):
            out_ref[0, f, :, pl.ds(j * LANES, LANES)] = jnp.concatenate(sums[f], axis=0).astype(
                jnp.bfloat16
            )


def fir(delays, voltages, prototype):
    parts, elems, samples = voltages.shape
    taps, chan = prototype.shape
    rows = 16
    window = (FRAMES + taps - 1) * chan
    return pl.pallas_call(
        fir_kernel,
        grid=(parts, elems // rows),
        in_specs=[
            pl.BlockSpec(memory_space=pltpu.SMEM),
            pl.BlockSpec((1, rows, samples), lambda r, g: (r, g, 0)),
            pl.BlockSpec((taps, chan), lambda r, g: (0, 0)),
        ],
        out_specs=pl.BlockSpec((1, FRAMES, rows, chan), lambda r, g: (r, 0, g, 0)),
        out_shape=jax.ShapeDtypeStruct((parts, FRAMES, elems, chan), jnp.bfloat16),
        scratch_shapes=[
            pltpu.VMEM((rows // 8, 8, window), jnp.float32),
            pltpu.VMEM((taps, 8, chan), jnp.float32),
        ],
        compiler_params=pltpu.CompilerParams(
            dimension_semantics=("arbitrary", "arbitrary"), vmem_limit_bytes=24 * 2**20
        ),
    )(delays, voltages, prototype)


def cosine(turns, chan):
    y = jnp.abs(turns % chan - chan // 2) - chan // 4
    x = y.astype(jnp.float32) * (2.0 * math.pi / chan)
    s = x * x
    poly = 1.0 / 362880 - s * (1.0 / 39916800)
    poly = -1.0 / 5040 + s * poly
    poly = 1.0 / 120 + s * poly
    poly = -1.0 / 6 + s * poly
    return (x + x * s * poly) * (chan**-0.5)


def split(value):
    high = value.astype(jnp.bfloat16)
    return high, (value - high.astype(jnp.float32)).astype(jnp.bfloat16)


NT = (((1,), (1,)), ((), ()))


def eight_points(x):
    def add(a, b):
        return (a[0] + b[0], a[1] + b[1])

    def sub(a, b):
        return (a[0] - b[0], a[1] - b[1])

    def minus_i(a):
        return (a[1], -a[0])

    def four(v):
        a, b = add(v[0], v[2]), sub(v[0], v[2])
        c, d = add(v[1], v[3]), minus_i(sub(v[1], v[3]))
        return [add(a, c), add(b, d), sub(a, c), sub(b, d)]

    root = math.sqrt(0.5)
    even = four([add(x[a], x[a + 4]) for a in range(4)])
    d = [sub(x[a], x[a + 4]) for a in range(4)]
    d1 = ((d[1][0] + d[1][1]) * root, (d[1][1] - d[1][0]) * root)
    d3 = ((d[3][1] - d[3][0]) * root, (-d[3][0] - d[3][1]) * root)
    odd = four([d[0], d1, minus_i(d[2]), d3])
    out = []
    for e, o in zip(even, odd):
        out += [e, o]
    return out


def beam_kernel(
    nelem,
    nchan,
    map_ref,
    wave_ref,
    weight_hbm,
    basis_hbm,
    power_ref,
    beam_ref,
    weight_ref,
    basis_ref,
    send_ref,
    recv_ref,
    picked_ref,
    local_sem,
    send_sem,
    recv_sem,
):
    parts, frames, elems, chan = wave_ref.shape
    count = nelem * nchan
    elem_at, chan_at = lax.axis_index("elem"), lax.axis_index("chan")
    me = elem_at * nchan + chan_at
    barrier = pltpu.get_barrier_semaphore()

    def partner(i):
        other = lax.rem(me + i, count)
        return other // nchan, lax.rem(other, nchan)

    def greet(i, carry):
        e, c = partner(i)
        pl.semaphore_signal(barrier, inc=1, device_id=(e, c), device_id_type=MESH)
        return carry

    lax.fori_loop(1, count, greet, 0)
    basis_copy = pltpu.make_async_copy(basis_hbm, basis_ref, local_sem.at[0])
    weight_copy = pltpu.make_async_copy(weight_hbm, weight_ref, local_sem.at[1])
    basis_copy.start()
    weight_copy.start()

    subbands = map_ref.shape[0]
    block = subbands // nchan
    rows = 2 * subbands
    row = lax.broadcasted_iota(jnp.int32, (rows, LANES), 0)
    band = (row // (2 * block)) * block + row % block
    wanted = jnp.zeros((rows, LANES), jnp.int32)
    for s in range(subbands):
        wanted = jnp.where(band == s, map_ref[s], wanted)
    quarter = ((row // block) % 2) * (chan // 4)
    lane = lax.broadcasted_iota(jnp.int32, (rows, LANES), 1)
    real_basis, imag_basis = [], []
    for j in range(chan // LANES):
        turns = wanted * (lane + j * LANES) + quarter
        real_basis.append(cosine(turns, chan))
        imag_basis.append(cosine(turns + 3 * (chan // 4), chan))
    real_basis = split(jnp.concatenate(real_basis, axis=1))
    imag_basis = split(jnp.concatenate(imag_basis, axis=1))
    wave = [wave_ref[r].reshape(frames * elems, chan) for r in range(2)]
    chosen = jnp.zeros((rows, frames * elems), jnp.float32)
    for r, basis in ((0, real_basis), (1, imag_basis)):
        for piece in basis:
            chosen = chosen + lax.dot_general(
                piece, wave[r], NT, preferred_element_type=jnp.float32
            )
    chosen = chosen.astype(jnp.bfloat16)
    for c in range(nchan):
        send_ref[c] = chosen[2 * block * c : 2 * block * (c + 1)]

    pl.semaphore_wait(barrier, count - 1)

    def send(i, carry):
        e, c = partner(i)
        pltpu.make_async_remote_copy(
            src_ref=send_ref.at[c],
            dst_ref=recv_ref.at[me],
            send_sem=send_sem,
            recv_sem=recv_sem,
            device_id=(e, c),
            device_id_type=MESH,
        ).start()
        return carry

    lax.fori_loop(1, count, send, 0)
    recv_ref[me] = send_ref[chan_at]

    lanes = chan // RADIX
    split_wave = [
        tuple(wave[r][:, a * lanes : (a + 1) * lanes].astype(jnp.float32) for r in range(2))
        for a in range(RADIX)
    ]
    classes = eight_points(split_wave)
    basis_copy.wait()
    powers = []
    for c in range(RADIX):
        mixed = jnp.concatenate(classes[c], axis=1).astype(jnp.bfloat16)
        spec = jnp.dot(mixed, basis_ref[c], preferred_element_type=jnp.float32)
        both = spec[:, :lanes] * spec[:, :lanes] + spec[:, lanes:] * spec[:, lanes:]
        total = both[:elems]
        for f in range(1, frames):
            total = total + both[f * elems : (f + 1) * elems]
        powers.append(total * (1.0 / frames))
    wide = lanes // RADIX
    at = lax.broadcasted_iota(jnp.int32, (elems, lanes), 1)
    mixed = []
    for e in range(RADIX):
        piece = None
        for c in range(RADIX):
            shift = (wide * (c - e)) % lanes
            moved = pltpu.roll(powers[c], shift, 1) if shift else powers[c]
            piece = moved if piece is None else jnp.where(at // wide == c, moved, piece)
        mixed.append(piece)
    mixed = jnp.concatenate(mixed, axis=0).astype(jnp.bfloat16)
    down = lax.broadcasted_iota(jnp.int32, (lanes, lanes), 0)
    over = lax.broadcasted_iota(jnp.int32, (lanes, lanes), 1)
    order = (over == (down % wide) * RADIX + down // wide).astype(jnp.float32)
    final = jnp.dot(mixed, order.astype(jnp.bfloat16), preferred_element_type=jnp.float32)
    for e in range(RADIX):
        power_ref[:, e * lanes : (e + 1) * lanes] = final[e * elems : (e + 1) * elems].astype(
            jnp.bfloat16
        )

    weight_rows = weight_ref.shape[0]
    beams = weight_rows // (2 * block)
    down = lax.broadcasted_iota(jnp.int32, (weight_rows, 2 * beams), 0)
    over = lax.broadcasted_iota(jnp.int32, (weight_rows, 2 * beams), 1)
    gather = (down // (2 * block) == over % beams) & ((down // block) % 2 == over // beams)
    gather = gather.astype(jnp.float32).astype(jnp.bfloat16)
    weight_copy.wait()

    arrived = recv_ref.at[pl.ds(0, count - 1)]
    pltpu.make_async_copy(arrived, arrived, recv_sem).wait()

    group = LANES // elems
    inside = lax.broadcasted_iota(jnp.int32, (2 * block, LANES), 1) // elems

    def place(q, carry):
        tiles = [recv_ref[q * group + i].astype(jnp.float32) for i in range(group)]
        pieces = []
        for f in range(frames):
            piece = None
            for i in range(group):
                shift = (elems * (i - f)) % LANES
                moved = pltpu.roll(tiles[i], shift, 1) if shift else tiles[i]
                piece = moved if piece is None else jnp.where(inside == i, moved, piece)
            pieces.append(piece)
        where = pl.multiple_of(q * LANES, LANES)
        picked_ref[:, pl.ds(where, LANES)] = jnp.concatenate(pieces, axis=0).astype(jnp.bfloat16)
        return carry

    steps = count // group
    if steps <= 8:
        for q in range(steps):
            place(q, 0)
    else:
        lax.fori_loop(0, steps, place, 0)
    product = lax.dot_general(
        picked_ref[...], weight_ref[...], NT, preferred_element_type=jnp.float32
    )
    at = lax.broadcasted_iota(jnp.int32, product.shape, 1)
    row = lax.broadcasted_iota(jnp.int32, product.shape, 0)
    product = jnp.where(at % block == row % block, product, 0.0)
    high, low = split(product)
    summed = jnp.dot(high, gather, preferred_element_type=jnp.float32) + jnp.dot(
        low, gather, preferred_element_type=jnp.float32
    )
    for f in range(frames):
        top = summed[2 * block * f : 2 * block * f + block]
        bottom = summed[2 * block * f + block : 2 * block * (f + 1)]
        real = top[:, :beams] - bottom[:, beams:]
        imag = bottom[:, :beams] + top[:, beams:]
        for s in range(block):
            beam_ref[0, pl.ds(s * frames + f, 1), :] = real[s : s + 1]
            beam_ref[1, pl.ds(s * frames + f, 1), :] = imag[s : s + 1]

    pltpu.make_async_copy(arrived, arrived, send_sem).wait()


def class_basis(chan):
    lanes = chan // RADIX
    b = np.arange(lanes)[:, None]
    d = np.arange(lanes)[None, :]
    out = []
    for c in range(RADIX):
        angle = 2.0 * np.pi / chan * (b * (c + RADIX * d) % chan)
        cos, sin = np.cos(angle) * chan**-0.5, np.sin(angle) * chan**-0.5
        out.append(np.block([[cos, -sin], [sin, cos]]))
    return jnp.asarray(np.stack(out), jnp.bfloat16)


def on_device(nelem, nchan, voltages, delays, prototype, subband_map, beam_weights):
    wave = fir(delays, voltages, prototype)
    parts, frames, elems, chan = wave.shape
    beams, _, block, total = beam_weights.shape
    weights = beam_weights.reshape(beams * 2 * block, total)
    basis = class_basis(chan)
    count = nelem * nchan
    return pl.pallas_call(
        functools.partial(beam_kernel, nelem, nchan),
        in_specs=[
            pl.BlockSpec(memory_space=pltpu.SMEM),
            pl.BlockSpec(memory_space=pltpu.VMEM),
            pl.BlockSpec(memory_space=pl.ANY),
            pl.BlockSpec(memory_space=pl.ANY),
        ],
        out_specs=[pl.BlockSpec(memory_space=pltpu.VMEM)] * 2,
        out_shape=[
            jax.ShapeDtypeStruct((elems, chan), jnp.bfloat16),
            jax.ShapeDtypeStruct((2, block * frames, beams), jnp.float32),
        ],
        scratch_shapes=[
            pltpu.VMEM(weights.shape, jnp.bfloat16),
            pltpu.VMEM(basis.shape, jnp.bfloat16),
            pltpu.VMEM((nchan, 2 * block, frames * elems), jnp.bfloat16),
            pltpu.VMEM((count, 2 * block, frames * elems), jnp.bfloat16),
            pltpu.VMEM((2 * block * frames, total), jnp.bfloat16),
            pltpu.SemaphoreType.DMA((2,)),
            pltpu.SemaphoreType.DMA,
            pltpu.SemaphoreType.DMA,
        ],
        compiler_params=pltpu.CompilerParams(collective_id=0, has_side_effects=True),
    )(subband_map, wave, weights, basis)


def solution(mesh):
    return jax.shard_map(
        functools.partial(on_device, mesh.shape["elem"], mesh.shape["chan"]),
        mesh=mesh,
        in_specs=(
            P(None, ("elem", "chan"), None),
            P(("elem", "chan")),
            P(),
            P(),
            P("elem", None, "chan", None),
        ),
        out_specs=(P(("elem", "chan"), None), P(None, "chan", "elem")),
        check_vma=False,
    )
```

```python
import functools
import math

import jax
import jax.numpy as jnp
import numpy as np
from jax import lax
from jax.experimental import pallas as pl
from jax.experimental.pallas import tpu as pltpu
from jax.sharding import PartitionSpec as P

FRAMES = 4
LANES = 128
RADIX = 8
MESH = pl.DeviceIdType.MESH


def cosine(turns, chan):
    y = jnp.abs(turns % chan - chan // 2) - chan // 4
    x = y.astype(jnp.float32) * (2.0 * math.pi / chan)
    s = x * x
    poly = 1.0 / 362880 - s * (1.0 / 39916800)
    poly = -1.0 / 5040 + s * poly
    poly = 1.0 / 120 + s * poly
    poly = -1.0 / 6 + s * poly
    return (x + x * s * poly) * (chan**-0.5)


def split(value):
    high = value.astype(jnp.bfloat16)
    return high, (value - high.astype(jnp.float32)).astype(jnp.bfloat16)


NT = (((1,), (1,)), ((), ()))


def eight_points(x):
    def add(a, b):
        return (a[0] + b[0], a[1] + b[1])

    def sub(a, b):
        return (a[0] - b[0], a[1] - b[1])

    def minus_i(a):
        return (a[1], -a[0])

    def four(v):
        a, b = add(v[0], v[2]), sub(v[0], v[2])
        c, d = add(v[1], v[3]), minus_i(sub(v[1], v[3]))
        return [add(a, c), add(b, d), sub(a, c), sub(b, d)]

    root = math.sqrt(0.5)
    even = four([add(x[a], x[a + 4]) for a in range(4)])
    d = [sub(x[a], x[a + 4]) for a in range(4)]
    d1 = ((d[1][0] + d[1][1]) * root, (d[1][1] - d[1][0]) * root)
    d3 = ((d[3][1] - d[3][0]) * root, (-d[3][0] - d[3][1]) * root)
    odd = four([d[0], d1, minus_i(d[2]), d3])
    out = []
    for e, o in zip(even, odd):
        out += [e, o]
    return out


def filter_chunk(chunk, groups, volt_ref, delay_ref, coef_ref, seg_ref, wave_ref):
    rows = volt_ref.shape[1]
    taps, _, chan = coef_ref.shape
    per = chan // LANES
    blocks = FRAMES + taps - 1
    part, group = chunk // groups, lax.rem(chunk, groups)
    lane = lax.broadcasted_iota(jnp.int32, (8, LANES), 1)
    sub = lax.broadcasted_iota(jnp.int32, (8, LANES), 0)
    halves = rows // 8
    index, keep = [], []
    for h in range(halves):
        shift = jnp.zeros((8, LANES), jnp.int32)
        for i in range(8):
            shift = jnp.where(sub == i, delay_ref[group * rows + h * 8 + i], shift)
        index.append((lane + shift) % LANES)
        keep.append(lane < LANES - shift)

    def turned(c):
        both = volt_ref[chunk, :, pl.ds(c * LANES, LANES)].astype(jnp.float32)
        return [
            jnp.take_along_axis(
                both[8 * h : 8 * h + 8], index[h], axis=1, mode="promise_in_bounds"
            )
            for h in range(halves)
        ]

    now = turned(0)
    for c in range(blocks * per):
        nxt = turned(c + 1)
        for h in range(halves):
            seg_ref[h, :, pl.ds(c * LANES, LANES)] = jnp.where(keep[h], now[h], nxt[h])
        now = nxt
    where = pl.multiple_of(group * rows, rows)
    for j in range(per):
        sums = [[None] * halves for _ in range(FRAMES)]
        for h in range(halves):
            held = [seg_ref[h, :, pl.ds((b * per + j) * LANES, LANES)] for b in range(blocks)]
            for t in range(taps):
                coef = coef_ref[t, :, pl.ds(j * LANES, LANES)]
                for f in range(FRAMES):
                    term = coef * held[f + t]
                    sums[f][h] = term if t == 0 else sums[f][h] + term
        for f in range(FRAMES):
            wave_ref[part, f, pl.ds(where, rows), pl.ds(j * LANES, LANES)] = jnp.concatenate(
                sums[f], axis=0
            ).astype(jnp.bfloat16)


def main_kernel(
    nelem,
    nchan,
    delay_hbm,
    map_hbm,
    volt_hbm,
    proto_hbm,
    weight_hbm,
    basis_hbm,
    power_ref,
    beam_ref,
    delay_ref,
    map_ref,
    volt_ref,
    proto_ref,
    raw_ref,
    basis_ref,
    seg_ref,
    coef_ref,
    wave_ref,
    weight_ref,
    send_ref,
    recv_ref,
    picked_ref,
    local_sem,
    volt_sem,
    send_sem,
    recv_sem,
):
    parts, frames, elems, chan = wave_ref.shape
    chunks, chunk_rows, _ = volt_ref.shape
    groups = chunks // parts
    taps = proto_ref.shape[0]
    count = nelem * nchan
    elem_at, chan_at = lax.axis_index("elem"), lax.axis_index("chan")
    me = elem_at * nchan + chan_at
    barrier = pltpu.get_barrier_semaphore()

    def partner(i):
        other = lax.rem(me + i, count)
        return other // nchan, lax.rem(other, nchan)

    map_copy = pltpu.make_async_copy(map_hbm, map_ref, local_sem.at[0])
    proto_copy = pltpu.make_async_copy(proto_hbm, proto_ref, local_sem.at[1])
    delay_copy = pltpu.make_async_copy(delay_hbm, delay_ref, local_sem.at[2])
    basis_copy = pltpu.make_async_copy(basis_hbm, basis_ref, local_sem.at[3])
    weight_copy = pltpu.make_async_copy(weight_hbm, raw_ref, local_sem.at[4])
    volt_copies = [
        pltpu.make_async_copy(
            volt_hbm.at[k // groups, pl.ds(k % groups * chunk_rows, chunk_rows)],
            volt_ref.at[k],
            volt_sem.at[k],
        )
        for k in range(chunks)
    ]
    map_copy.start()
    proto_copy.start()
    delay_copy.start()
    for copy in volt_copies:
        copy.start()
    basis_copy.start()
    weight_copy.start()

    def greet(i, carry):
        e, c = partner(i)
        pl.semaphore_signal(barrier, inc=1, device_id=(e, c), device_id_type=MESH)
        return carry

    lax.fori_loop(1, count, greet, 0)
    map_copy.wait()

    subbands = map_ref.shape[0]
    block = subbands // nchan
    rows = 2 * subbands
    row = lax.broadcasted_iota(jnp.int32, (rows, LANES), 0)
    band = (row // (2 * block)) * block + row % block
    wanted = jnp.zeros((rows, LANES), jnp.int32)
    for s in range(subbands):
        wanted = jnp.where(band == s, map_ref[s], wanted)
    quarter = ((row // block) % 2) * (chan // 4)
    lane = lax.broadcasted_iota(jnp.int32, (rows, LANES), 1)
    real_basis, imag_basis = [], []
    for j in range(chan // LANES):
        turns = wanted * (lane + j * LANES) + quarter
        real_basis.append(cosine(turns, chan))
        imag_basis.append(cosine(turns + 3 * (chan // 4), chan))
    real_basis = split(jnp.concatenate(real_basis, axis=1))
    imag_basis = split(jnp.concatenate(imag_basis, axis=1))
    proto_copy.wait()
    for t in range(taps):
        coef_ref[t] = jnp.broadcast_to(
            proto_ref[pl.ds(t, 1), :].astype(jnp.float32), (8, chan)
        )
    delay_copy.wait()

    def filter_step(k, carry):
        pltpu.make_async_copy(
            volt_hbm.at[0, pl.ds(0, chunk_rows)], volt_ref.at[k], volt_sem.at[k]
        ).wait()
        filter_chunk(k, groups, volt_ref, delay_ref, coef_ref, seg_ref, wave_ref)
        return carry

    lax.fori_loop(0, chunks, filter_step, 0)
    wave = [wave_ref[r].reshape(frames * elems, chan) for r in range(2)]
    chosen = jnp.zeros((rows, frames * elems), jnp.float32)
    for r, basis in ((0, real_basis), (1, imag_basis)):
        for piece in basis:
            chosen = chosen + lax.dot_general(
                piece, wave[r], NT, preferred_element_type=jnp.float32
            )
    chosen = chosen.astype(jnp.bfloat16)
    for c in range(nchan):
        send_ref[c] = chosen[2 * block * c : 2 * block * (c + 1)]

    pl.semaphore_wait(barrier, count - 1)

    def send(i, carry):
        e, c = partner(i)
        pltpu.make_async_remote_copy(
            src_ref=send_ref.at[c],
            dst_ref=recv_ref.at[me],
            send_sem=send_sem,
            recv_sem=recv_sem,
            device_id=(e, c),
            device_id_type=MESH,
        ).start()
        return carry

    lax.fori_loop(1, count, send, 0)
    recv_ref[me] = send_ref[chan_at]

    lanes = chan // RADIX
    split_wave = [
        tuple(wave[r][:, a * lanes : (a + 1) * lanes].astype(jnp.float32) for r in range(2))
        for a in range(RADIX)
    ]
    classes = eight_points(split_wave)
    basis_copy.wait()
    powers = []
    for c in range(RADIX):
        mixed = jnp.concatenate(classes[c], axis=1).astype(jnp.bfloat16)
        spec = jnp.dot(mixed, basis_ref[c], preferred_element_type=jnp.float32)
        both = spec[:, :lanes] * spec[:, :lanes] + spec[:, lanes:] * spec[:, lanes:]
        total = both[:elems]
        for f in range(1, frames):
            total = total + both[f * elems : (f + 1) * elems]
        powers.append(total * (1.0 / frames))
    wide = lanes // RADIX
    at = lax.broadcasted_iota(jnp.int32, (elems, lanes), 1)
    mixed = []
    for e in range(RADIX):
        piece = None
        for c in range(RADIX):
            shift = (wide * (c - e)) % lanes
            moved = pltpu.roll(powers[c], shift, 1) if shift else powers[c]
            piece = moved if piece is None else jnp.where(at // wide == c, moved, piece)
        mixed.append(piece)
    mixed = jnp.concatenate(mixed, axis=0).astype(jnp.bfloat16)
    down = lax.broadcasted_iota(jnp.int32, (lanes, lanes), 0)
    over = lax.broadcasted_iota(jnp.int32, (lanes, lanes), 1)
    order = (over == (down % wide) * RADIX + down // wide).astype(jnp.float32)
    final = jnp.dot(mixed, order.astype(jnp.bfloat16), preferred_element_type=jnp.float32)
    for e in range(RADIX):
        power_ref[:, e * lanes : (e + 1) * lanes] = final[e * elems : (e + 1) * elems].astype(
            jnp.bfloat16
        )

    weight_rows = weight_ref.shape[0]
    beams = weight_rows // (2 * block)
    down = lax.broadcasted_iota(jnp.int32, (weight_rows, 2 * beams), 0)
    over = lax.broadcasted_iota(jnp.int32, (weight_rows, 2 * beams), 1)
    gather = (down // (2 * block) == over % beams) & ((down // block) % 2 == over // beams)
    gather = gather.astype(jnp.float32).astype(jnp.bfloat16)
    weight_copy.wait()
    step = min(8, raw_ref.shape[0])
    for i in range(0, raw_ref.shape[0], step):
        piece = raw_ref[i : i + step].reshape(step * 2 * block, raw_ref.shape[3])
        weight_ref[2 * block * i : 2 * block * (i + step)] = piece

    arrived = recv_ref.at[pl.ds(0, count - 1)]
    pltpu.make_async_copy(arrived, arrived, recv_sem).wait()

    group = LANES // elems
    inside = lax.broadcasted_iota(jnp.int32, (2 * block, LANES), 1) // elems

    def place(q, carry):
        tiles = [recv_ref[q * group + i].astype(jnp.float32) for i in range(group)]
        pieces = []
        for f in range(frames):
            piece = None
            for i in range(group):
                shift = (elems * (i - f)) % LANES
                moved = pltpu.roll(tiles[i], shift, 1) if shift else tiles[i]
                piece = moved if piece is None else jnp.where(inside == i, moved, piece)
            pieces.append(piece)
        where = pl.multiple_of(q * LANES, LANES)
        picked_ref[:, pl.ds(where, LANES)] = jnp.concatenate(pieces, axis=0).astype(jnp.bfloat16)
        return carry

    steps = count // group
    if steps <= 8:
        for q in range(steps):
            place(q, 0)
    else:
        lax.fori_loop(0, steps, place, 0)
    product = lax.dot_general(
        picked_ref[...], weight_ref[...], NT, preferred_element_type=jnp.float32
    )
    at = lax.broadcasted_iota(jnp.int32, product.shape, 1)
    row = lax.broadcasted_iota(jnp.int32, product.shape, 0)
    product = jnp.where(at % block == row % block, product, 0.0)
    high, low = split(product)
    summed = jnp.dot(high, gather, preferred_element_type=jnp.float32) + jnp.dot(
        low, gather, preferred_element_type=jnp.float32
    )
    for f in range(frames):
        top = summed[2 * block * f : 2 * block * f + block]
        bottom = summed[2 * block * f + block : 2 * block * (f + 1)]
        real = top[:, :beams] - bottom[:, beams:]
        imag = bottom[:, :beams] + top[:, beams:]
        for s in range(block):
            beam_ref[0, pl.ds(s * frames + f, 1), :] = real[s : s + 1]
            beam_ref[1, pl.ds(s * frames + f, 1), :] = imag[s : s + 1]

    pltpu.make_async_copy(arrived, arrived, send_sem).wait()


def class_basis(chan):
    lanes = chan // RADIX
    b = np.arange(lanes)[:, None]
    d = np.arange(lanes)[None, :]
    out = []
    for c in range(RADIX):
        angle = 2.0 * np.pi / chan * (b * (c + RADIX * d) % chan)
        cos, sin = np.cos(angle) * chan**-0.5, np.sin(angle) * chan**-0.5
        out.append(np.block([[cos, -sin], [sin, cos]]))
    return jnp.asarray(np.stack(out), jnp.bfloat16)


def deliver_kernel(power_from, beam_from, power_to, beam_to, sems):
    copies = [
        pltpu.make_async_copy(power_from, power_to, sems.at[0]),
        pltpu.make_async_copy(beam_from, beam_to, sems.at[1]),
    ]
    for copy in copies:
        copy.start()
    for copy in copies:
        copy.wait()


def on_device(nelem, nchan, voltages, delays, prototype, subband_map, beam_weights):
    parts, elems, samples = voltages.shape
    taps, chan = prototype.shape
    beams, _, block, total = beam_weights.shape
    window = (FRAMES + taps - 1) * chan
    basis = class_basis(chan)
    count = nelem * nchan
    rows = 16
    chunks = parts * elems // rows
    out_shape = [
        jax.ShapeDtypeStruct((elems, chan), jnp.bfloat16),
        jax.ShapeDtypeStruct((2, block * FRAMES, beams), jnp.float32),
    ]
    power, beam = pl.pallas_call(
        functools.partial(main_kernel, nelem, nchan),
        in_specs=[pl.BlockSpec(memory_space=pltpu.HBM)] * 6,
        out_specs=[pl.BlockSpec(memory_space=pltpu.VMEM)] * 2,
        out_shape=[pltpu.VMEM(o.shape, o.dtype) for o in out_shape],
        scratch_shapes=[
            pltpu.SMEM(delays.shape, jnp.int32),
            pltpu.SMEM(subband_map.shape, jnp.int32),
            pltpu.VMEM((chunks, rows, samples), jnp.bfloat16),
            pltpu.VMEM((taps, chan), jnp.bfloat16),
            pltpu.VMEM(beam_weights.shape, jnp.bfloat16),
            pltpu.VMEM(basis.shape, jnp.bfloat16),
            pltpu.VMEM((rows // 8, 8, window), jnp.float32),
            pltpu.VMEM((taps, 8, chan), jnp.float32),
            pltpu.VMEM((parts, FRAMES, elems, chan), jnp.bfloat16),
            pltpu.VMEM((beams * 2 * block, total), jnp.bfloat16),
            pltpu.VMEM((nchan, 2 * block, FRAMES * elems), jnp.bfloat16),
            pltpu.VMEM((count, 2 * block, FRAMES * elems), jnp.bfloat16),
            pltpu.VMEM((2 * block * FRAMES, total), jnp.bfloat16),
            pltpu.SemaphoreType.DMA((5,)),
            pltpu.SemaphoreType.DMA((chunks,)),
            pltpu.SemaphoreType.DMA,
            pltpu.SemaphoreType.DMA,
        ],
        compiler_params=pltpu.CompilerParams(
            collective_id=0, has_side_effects=True, vmem_limit_bytes=66_400_000
        ),
    )(delays, subband_map, voltages, prototype, beam_weights, basis)
    return pl.pallas_call(
        deliver_kernel,
        in_specs=[pl.BlockSpec(memory_space=pl.ANY)] * 2,
        out_specs=[pl.BlockSpec(memory_space=pl.ANY)] * 2,
        out_shape=out_shape,
        scratch_shapes=[pltpu.SemaphoreType.DMA((2,))],
        compiler_params=pltpu.CompilerParams(vmem_limit_bytes=2**20),
    )(power, beam)


def solution(mesh):
    return jax.shard_map(
        functools.partial(on_device, mesh.shape["elem"], mesh.shape["chan"]),
        mesh=mesh,
        in_specs=(
            P(None, ("elem", "chan"), None),
            P(("elem", "chan")),
            P(),
            P(),
            P("elem", None, "chan", None),
        ),
        out_specs=(P(("elem", "chan"), None), P(None, "chan", "elem")),
        check_vma=False,
    )
```

```python
import functools
import math

import jax
import jax.numpy as jnp
import numpy as np
from jax import lax
from jax.experimental import pallas as pl
from jax.experimental.pallas import tpu as pltpu
from jax.sharding import PartitionSpec as P

FRAMES = 4
LANES = 128
RADIX = 8
LOGICAL = pl.DeviceIdType.LOGICAL


def cosine(turns, chan):
    y = jnp.abs(turns % chan - chan // 2) - chan // 4
    x = y.astype(jnp.float32) * (2.0 * math.pi / chan)
    s = x * x
    poly = 1.0 / 362880 - s * (1.0 / 39916800)
    poly = -1.0 / 5040 + s * poly
    poly = 1.0 / 120 + s * poly
    poly = -1.0 / 6 + s * poly
    return (x + x * s * poly) * (chan**-0.5)


def split(value):
    high = value.astype(jnp.bfloat16)
    return high, (value - high.astype(jnp.float32)).astype(jnp.bfloat16)


NT = (((1,), (1,)), ((), ()))


def eight_points(x):
    def add(a, b):
        return (a[0] + b[0], a[1] + b[1])

    def sub(a, b):
        return (a[0] - b[0], a[1] - b[1])

    def minus_i(a):
        return (a[1], -a[0])

    def four(v):
        a, b = add(v[0], v[2]), sub(v[0], v[2])
        c, d = add(v[1], v[3]), minus_i(sub(v[1], v[3]))
        return [add(a, c), add(b, d), sub(a, c), sub(b, d)]

    root = math.sqrt(0.5)
    even = four([add(x[a], x[a + 4]) for a in range(4)])
    d = [sub(x[a], x[a + 4]) for a in range(4)]
    d1 = ((d[1][0] + d[1][1]) * root, (d[1][1] - d[1][0]) * root)
    d3 = ((d[3][1] - d[3][0]) * root, (-d[3][0] - d[3][1]) * root)
    odd = four([d[0], d1, minus_i(d[2]), d3])
    out = []
    for e, o in zip(even, odd):
        out += [e, o]
    return out


def filter_chunk(chunk, groups, volt_ref, delay_ref, coef_ref, seg_ref, wave_ref):
    rows = volt_ref.shape[1]
    taps, _, chan = coef_ref.shape
    per = chan // LANES
    blocks = FRAMES + taps - 1
    part, group = chunk // groups, lax.rem(chunk, groups)
    lane = lax.broadcasted_iota(jnp.int32, (8, LANES), 1)
    sub = lax.broadcasted_iota(jnp.int32, (8, LANES), 0)
    halves = rows // 8
    index, keep = [], []
    for h in range(halves):
        shift = jnp.zeros((8, LANES), jnp.int32)
        for i in range(8):
            shift = jnp.where(sub == i, delay_ref[group * rows + h * 8 + i], shift)
        index.append((lane + shift) % LANES)
        keep.append(lane < LANES - shift)

    def turned(c):
        both = volt_ref[chunk, :, pl.ds(c * LANES, LANES)].astype(jnp.float32)
        return [
            jnp.take_along_axis(
                both[8 * h : 8 * h + 8], index[h], axis=1, mode="promise_in_bounds"
            )
            for h in range(halves)
        ]

    now = turned(0)
    for c in range(blocks * per):
        nxt = turned(c + 1)
        for h in range(halves):
            seg_ref[h, :, pl.ds(c * LANES, LANES)] = jnp.where(keep[h], now[h], nxt[h])
        now = nxt
    where = pl.multiple_of(group * rows, rows)
    for j in range(per):
        sums = [[None] * halves for _ in range(FRAMES)]
        for h in range(halves):
            held = [seg_ref[h, :, pl.ds((b * per + j) * LANES, LANES)] for b in range(blocks)]
            for t in range(taps):
                coef = coef_ref[t, :, pl.ds(j * LANES, LANES)]
                for f in range(FRAMES):
                    term = coef * held[f + t]
                    sums[f][h] = term if t == 0 else sums[f][h] + term
        for f in range(FRAMES):
            wave_ref[part, f, pl.ds(where, rows), pl.ds(j * LANES, LANES)] = jnp.concatenate(
                sums[f], axis=0
            ).astype(jnp.bfloat16)


def main_kernel(
    nelem,
    nchan,
    delay_hbm,
    map_hbm,
    volt_hbm,
    proto_hbm,
    weight_hbm,
    basis_hbm,
    power_ref,
    beam_ref,
    delay_ref,
    map_ref,
    volt_ref,
    proto_ref,
    raw_ref,
    basis_ref,
    seg_ref,
    coef_ref,
    wave_ref,
    weight_ref,
    send_ref,
    recv_ref,
    picked_ref,
    local_sem,
    volt_sem,
    send_sem,
    recv_sem,
):
    parts, frames, elems, chan = wave_ref.shape
    chunks, chunk_rows, _ = volt_ref.shape
    groups = chunks // parts
    taps = proto_ref.shape[0]
    count = nelem * nchan
    elem_at, chan_at = lax.axis_index("elem"), lax.axis_index("chan")
    me = elem_at * nchan + chan_at
    barrier = pltpu.get_barrier_semaphore()

    def partner(i):
        other = me + i
        return jnp.where(other >= count, other - count, other)

    map_copy = pltpu.make_async_copy(map_hbm, map_ref, local_sem.at[0])
    proto_copy = pltpu.make_async_copy(proto_hbm, proto_ref, local_sem.at[1])
    delay_copy = pltpu.make_async_copy(delay_hbm, delay_ref, local_sem.at[2])
    basis_copy = pltpu.make_async_copy(basis_hbm, basis_ref, local_sem.at[3])
    weight_copy = pltpu.make_async_copy(weight_hbm, raw_ref, local_sem.at[4])
    volt_copies = [
        pltpu.make_async_copy(
            volt_hbm.at[k // groups, pl.ds(k % groups * chunk_rows, chunk_rows)],
            volt_ref.at[k],
            volt_sem.at[k],
        )
        for k in range(chunks)
    ]
    map_copy.start()
    proto_copy.start()
    delay_copy.start()
    for copy in volt_copies:
        copy.start()

    def greet(i, carry):
        pl.semaphore_signal(barrier, inc=1, device_id=partner(i), device_id_type=LOGICAL)
        return carry

    if count <= 64:
        for i in sorted(range(1, count), key=lambda i: -min(i, count - i)):
            greet(i, 0)
    else:
        lax.fori_loop(1, count, greet, 0)
    map_copy.wait()

    subbands = map_ref.shape[0]
    block = subbands // nchan
    rows = 2 * subbands
    row = lax.broadcasted_iota(jnp.int32, (rows, LANES), 0)
    band = (row // (2 * block)) * block + row % block
    wanted = jnp.zeros((rows, LANES), jnp.int32)
    for s in range(subbands):
        wanted = jnp.where(band == s, map_ref[s], wanted)
    quarter = ((row // block) % 2) * (chan // 4)
    lane = lax.broadcasted_iota(jnp.int32, (rows, LANES), 1)
    real_basis, imag_basis = [], []
    for j in range(chan // LANES):
        turns = wanted * (lane + j * LANES) + quarter
        real_basis.append(cosine(turns, chan))
        imag_basis.append(cosine(turns + 3 * (chan // 4), chan))
    real_basis = split(jnp.concatenate(real_basis, axis=1))
    imag_basis = split(jnp.concatenate(imag_basis, axis=1))
    proto_copy.wait()
    for t in range(taps):
        coef_ref[t] = jnp.broadcast_to(
            proto_ref[pl.ds(t, 1), :].astype(jnp.float32), (8, chan)
        )
    delay_copy.wait()

    def filter_step(k, carry):
        pltpu.make_async_copy(
            volt_hbm.at[0, pl.ds(0, chunk_rows)], volt_ref.at[k], volt_sem.at[k]
        ).wait()

        @pl.when(k == chunks - 1)
        def _():
            basis_copy.start()
            weight_copy.start()

        filter_chunk(k, groups, volt_ref, delay_ref, coef_ref, seg_ref, wave_ref)
        return carry

    lax.fori_loop(0, chunks, filter_step, 0)
    wave = [wave_ref[r].reshape(frames * elems, chan) for r in range(2)]
    chosen = jnp.zeros((rows, frames * elems), jnp.float32)
    for r, basis in ((0, real_basis), (1, imag_basis)):
        for piece in basis:
            chosen = chosen + lax.dot_general(
                piece, wave[r], NT, preferred_element_type=jnp.float32
            )
    chosen = chosen.astype(jnp.bfloat16)
    for c in range(nchan):
        send_ref[c] = chosen[2 * block * c : 2 * block * (c + 1)]

    pl.semaphore_wait(barrier, count - 1)

    def send(i, carry):
        other = partner(i)
        pltpu.make_async_remote_copy(
            src_ref=send_ref.at[lax.rem(other, nchan)],
            dst_ref=recv_ref.at[me],
            send_sem=send_sem,
            recv_sem=recv_sem,
            device_id=other,
            device_id_type=LOGICAL,
        ).start()
        return carry

    if count <= 64:
        for i in sorted(range(1, count), key=lambda i: -min(i, count - i)):
            send(i, 0)
    else:
        lax.fori_loop(1, count, send, 0)
    recv_ref[me] = send_ref[chan_at]

    lanes = chan // RADIX
    split_wave = [
        tuple(wave[r][:, a * lanes : (a + 1) * lanes].astype(jnp.float32) for r in range(2))
        for a in range(RADIX)
    ]
    classes = eight_points(split_wave)
    basis_copy.wait()
    powers = []
    for c in range(RADIX):
        mixed = jnp.concatenate(classes[c], axis=1).astype(jnp.bfloat16)
        spec = jnp.dot(mixed, basis_ref[c], preferred_element_type=jnp.float32)
        both = spec[:, :lanes] * spec[:, :lanes] + spec[:, lanes:] * spec[:, lanes:]
        total = both[:elems]
        for f in range(1, frames):
            total = total + both[f * elems : (f + 1) * elems]
        powers.append(total * (1.0 / frames))
    wide = lanes // RADIX
    at = lax.broadcasted_iota(jnp.int32, (elems, lanes), 1)
    mixed = []
    for e in range(RADIX):
        piece = None
        for c in range(RADIX):
            shift = (wide * (c - e)) % lanes
            moved = pltpu.roll(powers[c], shift, 1) if shift else powers[c]
            piece = moved if piece is None else jnp.where(at // wide == c, moved, piece)
        mixed.append(piece)
    mixed = jnp.concatenate(mixed, axis=0).astype(jnp.bfloat16)
    down = lax.broadcasted_iota(jnp.int32, (lanes, lanes), 0)
    over = lax.broadcasted_iota(jnp.int32, (lanes, lanes), 1)
    order = (over == (down % wide) * RADIX + down // wide).astype(jnp.float32)
    final = jnp.dot(mixed, order.astype(jnp.bfloat16), preferred_element_type=jnp.float32)
    for e in range(RADIX):
        power_ref[:, e * lanes : (e + 1) * lanes] = final[e * elems : (e + 1) * elems].astype(
            jnp.bfloat16
        )

    weight_rows = weight_ref.shape[0]
    beams = weight_rows // (2 * block)
    down = lax.broadcasted_iota(jnp.int32, (weight_rows, 2 * beams), 0)
    over = lax.broadcasted_iota(jnp.int32, (weight_rows, 2 * beams), 1)
    gather = (down // (2 * block) == over % beams) & ((down // block) % 2 == over // beams)
    gather = gather.astype(jnp.float32).astype(jnp.bfloat16)
    weight_copy.wait()
    step = min(8, raw_ref.shape[0])
    for i in range(0, raw_ref.shape[0], step):
        piece = raw_ref[i : i + step].reshape(step * 2 * block, raw_ref.shape[3])
        weight_ref[2 * block * i : 2 * block * (i + step)] = piece

    arrived = recv_ref.at[pl.ds(0, count - 1)]
    pltpu.make_async_copy(arrived, arrived, recv_sem).wait()

    group = LANES // elems
    inside = lax.broadcasted_iota(jnp.int32, (2 * block, LANES), 1) // elems

    def place(q, carry):
        tiles = [recv_ref[q * group + i].astype(jnp.float32) for i in range(group)]
        pieces = []
        for f in range(frames):
            piece = None
            for i in range(group):
                shift = (elems * (i - f)) % LANES
                moved = pltpu.roll(tiles[i], shift, 1) if shift else tiles[i]
                piece = moved if piece is None else jnp.where(inside == i, moved, piece)
            pieces.append(piece)
        where = pl.multiple_of(q * LANES, LANES)
        picked_ref[:, pl.ds(where, LANES)] = jnp.concatenate(pieces, axis=0).astype(jnp.bfloat16)
        return carry

    steps = count // group
    if steps <= 8:
        for q in range(steps):
            place(q, 0)
    else:
        lax.fori_loop(0, steps, place, 0)
    product = lax.dot_general(
        picked_ref[...], weight_ref[...], NT, preferred_element_type=jnp.float32
    )
    at = lax.broadcasted_iota(jnp.int32, product.shape, 1)
    row = lax.broadcasted_iota(jnp.int32, product.shape, 0)
    product = jnp.where(at % block == row % block, product, 0.0)
    high, low = split(product)
    summed = jnp.dot(high, gather, preferred_element_type=jnp.float32) + jnp.dot(
        low, gather, preferred_element_type=jnp.float32
    )
    for f in range(frames):
        top = summed[2 * block * f : 2 * block * f + block]
        bottom = summed[2 * block * f + block : 2 * block * (f + 1)]
        real = top[:, :beams] - bottom[:, beams:]
        imag = bottom[:, :beams] + top[:, beams:]
        for s in range(block):
            beam_ref[0, pl.ds(s * frames + f, 1), :] = real[s : s + 1]
            beam_ref[1, pl.ds(s * frames + f, 1), :] = imag[s : s + 1]

    pltpu.make_async_copy(arrived, arrived, send_sem).wait()


def class_basis(chan):
    lanes = chan // RADIX
    b = np.arange(lanes)[:, None]
    d = np.arange(lanes)[None, :]
    out = []
    for c in range(RADIX):
        angle = 2.0 * np.pi / chan * (b * (c + RADIX * d) % chan)
        cos, sin = np.cos(angle) * chan**-0.5, np.sin(angle) * chan**-0.5
        out.append(np.block([[cos, -sin], [sin, cos]]))
    return jnp.asarray(np.stack(out), jnp.bfloat16)


def deliver_kernel(power_from, beam_from, power_to, beam_to, sems):
    copies = [
        pltpu.make_async_copy(power_from, power_to, sems.at[0]),
        pltpu.make_async_copy(beam_from, beam_to, sems.at[1]),
    ]
    for copy in copies:
        copy.start()
    for copy in copies:
        copy.wait()


def on_device(nelem, nchan, voltages, delays, prototype, subband_map, beam_weights):
    parts, elems, samples = voltages.shape
    taps, chan = prototype.shape
    beams, _, block, total = beam_weights.shape
    window = (FRAMES + taps - 1) * chan
    basis = class_basis(chan)
    count = nelem * nchan
    rows = 16
    chunks = parts * elems // rows
    out_shape = [
        jax.ShapeDtypeStruct((elems, chan), jnp.bfloat16),
        jax.ShapeDtypeStruct((2, block * FRAMES, beams), jnp.float32),
    ]
    power, beam = pl.pallas_call(
        functools.partial(main_kernel, nelem, nchan),
        in_specs=[pl.BlockSpec(memory_space=pltpu.HBM)] * 6,
        out_specs=[pl.BlockSpec(memory_space=pltpu.VMEM)] * 2,
        out_shape=[pltpu.VMEM(o.shape, o.dtype) for o in out_shape],
        scratch_shapes=[
            pltpu.SMEM(delays.shape, jnp.int32),
            pltpu.SMEM(subband_map.shape, jnp.int32),
            pltpu.VMEM((chunks, rows, samples), jnp.bfloat16),
            pltpu.VMEM((taps, chan), jnp.bfloat16),
            pltpu.VMEM(beam_weights.shape, jnp.bfloat16),
            pltpu.VMEM(basis.shape, jnp.bfloat16),
            pltpu.VMEM((rows // 8, 8, window), jnp.float32),
            pltpu.VMEM((taps, 8, chan), jnp.float32),
            pltpu.VMEM((parts, FRAMES, elems, chan), jnp.bfloat16),
            pltpu.VMEM((beams * 2 * block, total), jnp.bfloat16),
            pltpu.VMEM((nchan, 2 * block, FRAMES * elems), jnp.bfloat16),
            pltpu.VMEM((count, 2 * block, FRAMES * elems), jnp.bfloat16),
            pltpu.VMEM((2 * block * FRAMES, total), jnp.bfloat16),
            pltpu.SemaphoreType.DMA((5,)),
            pltpu.SemaphoreType.DMA((chunks,)),
            pltpu.SemaphoreType.DMA,
            pltpu.SemaphoreType.DMA,
        ],
        compiler_params=pltpu.CompilerParams(
            collective_id=0, has_side_effects=True, vmem_limit_bytes=66_400_000
        ),
    )(delays, subband_map, voltages, prototype, beam_weights, basis)
    return pl.pallas_call(
        deliver_kernel,
        in_specs=[pl.BlockSpec(memory_space=pl.ANY)] * 2,
        out_specs=[pl.BlockSpec(memory_space=pl.ANY)] * 2,
        out_shape=out_shape,
        scratch_shapes=[pltpu.SemaphoreType.DMA((2,))],
        compiler_params=pltpu.CompilerParams(vmem_limit_bytes=2**20),
    )(power, beam)


def solution(mesh):
    return jax.shard_map(
        functools.partial(on_device, mesh.shape["elem"], mesh.shape["chan"]),
        mesh=mesh,
        in_specs=(
            P(None, ("elem", "chan"), None),
            P(("elem", "chan")),
            P(),
            P(),
            P("elem", None, "chan", None),
        ),
        out_specs=(P(("elem", "chan"), None), P(None, "chan", "elem")),
        check_vma=False,
    )
```

```python
import functools
import math

import jax
import jax.numpy as jnp
import numpy as np
from jax import lax
from jax.experimental import pallas as pl
from jax.experimental.pallas import tpu as pltpu
from jax.sharding import PartitionSpec as P

FRAMES = 4
LANES = 128
RADIX = 8
LOGICAL = pl.DeviceIdType.LOGICAL


def cosine(turns, chan):
    y = jnp.abs((turns & (chan - 1)) - chan // 2) - chan // 4
    x = y.astype(jnp.float32) * (2.0 * math.pi / chan)
    s = x * x
    poly = 1.0 / 362880 - s * (1.0 / 39916800)
    poly = -1.0 / 5040 + s * poly
    poly = 1.0 / 120 + s * poly
    poly = -1.0 / 6 + s * poly
    return (x + x * s * poly) * (chan**-0.5)


def split(value):
    high = value.astype(jnp.bfloat16)
    return high, (value - high.astype(jnp.float32)).astype(jnp.bfloat16)


NT = (((1,), (1,)), ((), ()))


def eight_points(x):
    def add(a, b):
        return (a[0] + b[0], a[1] + b[1])

    def sub(a, b):
        return (a[0] - b[0], a[1] - b[1])

    def minus_i(a):
        return (a[1], -a[0])

    def four(v):
        a, b = add(v[0], v[2]), sub(v[0], v[2])
        c, d = add(v[1], v[3]), minus_i(sub(v[1], v[3]))
        return [add(a, c), add(b, d), sub(a, c), sub(b, d)]

    root = math.sqrt(0.5)
    even = four([add(x[a], x[a + 4]) for a in range(4)])
    d = [sub(x[a], x[a + 4]) for a in range(4)]
    d1 = ((d[1][0] + d[1][1]) * root, (d[1][1] - d[1][0]) * root)
    d3 = ((d[3][1] - d[3][0]) * root, (-d[3][0] - d[3][1]) * root)
    odd = four([d[0], d1, minus_i(d[2]), d3])
    out = []
    for e, o in zip(even, odd):
        out += [e, o]
    return out


def filter_chunk(chunk, groups, volt_ref, delay_ref, coef_ref, seg_ref, wave_ref):
    rows = volt_ref.shape[1]
    taps, _, chan = coef_ref.shape
    per = chan // LANES
    blocks = FRAMES + taps - 1
    part, group = chunk // groups, lax.rem(chunk, groups)
    lane = lax.broadcasted_iota(jnp.int32, (8, LANES), 1)
    sub = lax.broadcasted_iota(jnp.int32, (8, LANES), 0)
    halves = rows // 8
    index, keep = [], []
    for h in range(halves):
        shift = jnp.zeros((8, LANES), jnp.int32)
        for i in range(8):
            shift = jnp.where(sub == i, delay_ref[group * rows + h * 8 + i], shift)
        index.append((lane + shift) & (LANES - 1))
        keep.append(lane < LANES - shift)

    def turned(c):
        both = volt_ref[chunk, :, pl.ds(c * LANES, LANES)].astype(jnp.float32)
        return [
            jnp.take_along_axis(
                both[8 * h : 8 * h + 8], index[h], axis=1, mode="promise_in_bounds"
            )
            for h in range(halves)
        ]

    now = turned(0)
    for c in range(blocks * per):
        nxt = turned(c + 1)
        for h in range(halves):
            seg_ref[h, :, pl.ds(c * LANES, LANES)] = jnp.where(keep[h], now[h], nxt[h])
        now = nxt
    where = pl.multiple_of(group * rows, rows)
    for j in range(per):
        sums = [[None] * halves for _ in range(FRAMES)]
        for h in range(halves):
            held = [seg_ref[h, :, pl.ds((b * per + j) * LANES, LANES)] for b in range(blocks)]
            for t in range(taps):
                coef = coef_ref[t, :, pl.ds(j * LANES, LANES)]
                for f in range(FRAMES):
                    term = coef * held[f + t]
                    sums[f][h] = term if t == 0 else sums[f][h] + term
        for f in range(FRAMES):
            wave_ref[part, f, pl.ds(where, rows), pl.ds(j * LANES, LANES)] = jnp.concatenate(
                sums[f], axis=0
            ).astype(jnp.bfloat16)


def main_kernel(
    nelem,
    nchan,
    delay_hbm,
    map_hbm,
    volt_hbm,
    proto_hbm,
    weight_hbm,
    basis_hbm,
    power_ref,
    beam_ref,
    delay_ref,
    map_ref,
    volt_ref,
    proto_ref,
    raw_ref,
    basis_ref,
    seg_ref,
    coef_ref,
    wave_ref,
    weight_ref,
    send_ref,
    recv_ref,
    picked_ref,
    local_sem,
    volt_sem,
    send_sem,
    recv_sem,
):
    parts, frames, elems, chan = wave_ref.shape
    chunks, chunk_rows, _ = volt_ref.shape
    groups = chunks // parts
    taps = proto_ref.shape[0]
    count = nelem * nchan
    elem_at, chan_at = lax.axis_index("elem"), lax.axis_index("chan")
    me = elem_at * nchan + chan_at
    barrier = pltpu.get_barrier_semaphore()

    def each_partner(act):
        near_start = elem_at < nelem // 2

        def row(k, carry):
            first = jnp.where(near_start, nelem - 1 - k, k) * nchan
            for c in range(nchan):

                @pl.when(first + c != me)
                def _():
                    act(first + c, c)

            return carry

        if count <= 64:
            for k in range(nelem):
                row(k, 0)
        else:
            lax.fori_loop(0, nelem, row, 0)

    map_copy = pltpu.make_async_copy(map_hbm, map_ref, local_sem.at[0])
    proto_copy = pltpu.make_async_copy(proto_hbm, proto_ref, local_sem.at[1])
    delay_copy = pltpu.make_async_copy(delay_hbm, delay_ref, local_sem.at[2])
    basis_copy = pltpu.make_async_copy(basis_hbm, basis_ref, local_sem.at[3])
    weight_copy = pltpu.make_async_copy(weight_hbm, raw_ref, local_sem.at[4])
    volt_copies = [
        pltpu.make_async_copy(
            volt_hbm.at[k // groups, pl.ds(k % groups * chunk_rows, chunk_rows)],
            volt_ref.at[k],
            volt_sem.at[k],
        )
        for k in range(chunks)
    ]
    map_copy.start()
    proto_copy.start()
    delay_copy.start()
    for copy in volt_copies:
        copy.start()

    def greet(other, c):
        pl.semaphore_signal(barrier, inc=1, device_id=other, device_id_type=LOGICAL)

    each_partner(greet)
    map_copy.wait()

    subbands = map_ref.shape[0]
    block = subbands // nchan
    rows = 2 * subbands
    row = lax.broadcasted_iota(jnp.int32, (rows, LANES), 0)
    band = (row // (2 * block)) * block + row % block
    wanted = jnp.zeros((rows, LANES), jnp.int32)
    for s in range(subbands):
        wanted = jnp.where(band == s, map_ref[s], wanted)
    quarter = ((row // block) % 2) * (chan // 4)
    lane = lax.broadcasted_iota(jnp.int32, (rows, LANES), 1)
    real_basis, imag_basis = [], []
    for j in range(chan // LANES):
        turns = wanted * (lane + j * LANES) + quarter
        real_basis.append(cosine(turns, chan))
        imag_basis.append(cosine(turns + 3 * (chan // 4), chan))
    real_basis = split(jnp.concatenate(real_basis, axis=1))
    imag_basis = split(jnp.concatenate(imag_basis, axis=1))
    proto_copy.wait()
    for t in range(taps):
        coef_ref[t] = jnp.broadcast_to(
            proto_ref[pl.ds(t, 1), :].astype(jnp.float32), (8, chan)
        )
    delay_copy.wait()

    def filter_step(k, carry):
        pltpu.make_async_copy(
            volt_hbm.at[0, pl.ds(0, chunk_rows)], volt_ref.at[k], volt_sem.at[k]
        ).wait()

        @pl.when(k == chunks - 1)
        def _():
            basis_copy.start()
            weight_copy.start()

        filter_chunk(k, groups, volt_ref, delay_ref, coef_ref, seg_ref, wave_ref)
        return carry

    lax.fori_loop(0, chunks, filter_step, 0)
    wave = [wave_ref[r].reshape(frames * elems, chan) for r in range(2)]
    chosen = jnp.zeros((rows, frames * elems), jnp.float32)
    for r, basis in ((0, real_basis), (1, imag_basis)):
        for piece in basis:
            chosen = chosen + lax.dot_general(
                piece, wave[r], NT, preferred_element_type=jnp.float32
            )
    chosen = chosen.astype(jnp.bfloat16)
    for c in range(nchan):
        send_ref[c] = chosen[2 * block * c : 2 * block * (c + 1)]

    pl.semaphore_wait(barrier, count - 1)

    def send(other, c):
        pltpu.make_async_remote_copy(
            src_ref=send_ref.at[c],
            dst_ref=recv_ref.at[me],
            send_sem=send_sem,
            recv_sem=recv_sem,
            device_id=other,
            device_id_type=LOGICAL,
        ).start()

    each_partner(send)
    recv_ref[me] = send_ref[chan_at]

    lanes = chan // RADIX
    split_wave = [
        tuple(wave[r][:, a * lanes : (a + 1) * lanes].astype(jnp.float32) for r in range(2))
        for a in range(RADIX)
    ]
    classes = eight_points(split_wave)
    basis_copy.wait()
    powers = []
    for c in range(RADIX):
        mixed = jnp.concatenate(classes[c], axis=1).astype(jnp.bfloat16)
        spec = jnp.dot(mixed, basis_ref[c], preferred_element_type=jnp.float32)
        both = spec[:, :lanes] * spec[:, :lanes] + spec[:, lanes:] * spec[:, lanes:]
        total = both[:elems]
        for f in range(1, frames):
            total = total + both[f * elems : (f + 1) * elems]
        powers.append(total * (1.0 / frames))
    wide = lanes // RADIX
    at = lax.broadcasted_iota(jnp.int32, (elems, lanes), 1)
    mixed = []
    for e in range(RADIX):
        piece = None
        for c in range(RADIX):
            shift = (wide * (c - e)) % lanes
            moved = pltpu.roll(powers[c], shift, 1) if shift else powers[c]
            piece = moved if piece is None else jnp.where(at // wide == c, moved, piece)
        mixed.append(piece)
    mixed = jnp.concatenate(mixed, axis=0).astype(jnp.bfloat16)
    down = lax.broadcasted_iota(jnp.int32, (lanes, lanes), 0)
    over = lax.broadcasted_iota(jnp.int32, (lanes, lanes), 1)
    order = (over == (down % wide) * RADIX + down // wide).astype(jnp.float32)
    final = jnp.dot(mixed, order.astype(jnp.bfloat16), preferred_element_type=jnp.float32)
    for e in range(RADIX):
        power_ref[:, e * lanes : (e + 1) * lanes] = final[e * elems : (e + 1) * elems].astype(
            jnp.bfloat16
        )

    weight_rows = weight_ref.shape[0]
    beams = weight_rows // (2 * block)
    down = lax.broadcasted_iota(jnp.int32, (weight_rows, 2 * beams), 0)
    over = lax.broadcasted_iota(jnp.int32, (weight_rows, 2 * beams), 1)
    gather = (down // (2 * block) == over % beams) & ((down // block) % 2 == over // beams)
    gather = gather.astype(jnp.float32).astype(jnp.bfloat16)
    weight_copy.wait()
    step = min(8, raw_ref.shape[0])
    for i in range(0, raw_ref.shape[0], step):
        piece = raw_ref[i : i + step].reshape(step * 2 * block, raw_ref.shape[3])
        weight_ref[2 * block * i : 2 * block * (i + step)] = piece

    arrived = recv_ref.at[pl.ds(0, count - 1)]
    pltpu.make_async_copy(arrived, arrived, recv_sem).wait()

    group = LANES // elems
    inside = lax.broadcasted_iota(jnp.int32, (2 * block, LANES), 1) // elems

    def place(q, carry):
        tiles = [recv_ref[q * group + i].astype(jnp.float32) for i in range(group)]
        pieces = []
        for f in range(frames):
            piece = None
            for i in range(group):
                shift = (elems * (i - f)) % LANES
                moved = pltpu.roll(tiles[i], shift, 1) if shift else tiles[i]
                piece = moved if piece is None else jnp.where(inside == i, moved, piece)
            pieces.append(piece)
        where = pl.multiple_of(q * LANES, LANES)
        picked_ref[:, pl.ds(where, LANES)] = jnp.concatenate(pieces, axis=0).astype(jnp.bfloat16)
        return carry

    steps = count // group
    if steps <= 8:
        for q in range(steps):
            place(q, 0)
    else:
        lax.fori_loop(0, steps, place, 0)
    product = lax.dot_general(
        picked_ref[...], weight_ref[...], NT, preferred_element_type=jnp.float32
    )
    at = lax.broadcasted_iota(jnp.int32, product.shape, 1)
    row = lax.broadcasted_iota(jnp.int32, product.shape, 0)
    product = jnp.where(at % block == row % block, product, 0.0)
    high, low = split(product)
    summed = jnp.dot(high, gather, preferred_element_type=jnp.float32) + jnp.dot(
        low, gather, preferred_element_type=jnp.float32
    )
    for f in range(frames):
        top = summed[2 * block * f : 2 * block * f + block]
        bottom = summed[2 * block * f + block : 2 * block * (f + 1)]
        real = top[:, :beams] - bottom[:, beams:]
        imag = bottom[:, :beams] + top[:, beams:]
        for s in range(block):
            beam_ref[0, pl.ds(s * frames + f, 1), :] = real[s : s + 1]
            beam_ref[1, pl.ds(s * frames + f, 1), :] = imag[s : s + 1]

    pltpu.make_async_copy(arrived, arrived, send_sem).wait()


def class_basis(chan):
    lanes = chan // RADIX
    b = np.arange(lanes)[:, None]
    d = np.arange(lanes)[None, :]
    out = []
    for c in range(RADIX):
        angle = 2.0 * np.pi / chan * (b * (c + RADIX * d) % chan)
        cos, sin = np.cos(angle) * chan**-0.5, np.sin(angle) * chan**-0.5
        out.append(np.block([[cos, -sin], [sin, cos]]))
    return jnp.asarray(np.stack(out), jnp.bfloat16)


def deliver_kernel(power_from, beam_from, power_to, beam_to, sems):
    copies = [
        pltpu.make_async_copy(power_from, power_to, sems.at[0]),
        pltpu.make_async_copy(beam_from, beam_to, sems.at[1]),
    ]
    for copy in copies:
        copy.start()
    for copy in copies:
        copy.wait()


def on_device(nelem, nchan, voltages, delays, prototype, subband_map, beam_weights):
    parts, elems, samples = voltages.shape
    taps, chan = prototype.shape
    beams, _, block, total = beam_weights.shape
    window = (FRAMES + taps - 1) * chan
    basis = class_basis(chan)
    count = nelem * nchan
    rows = 16
    chunks = parts * elems // rows
    out_shape = [
        jax.ShapeDtypeStruct((elems, chan), jnp.bfloat16),
        jax.ShapeDtypeStruct((2, block * FRAMES, beams), jnp.float32),
    ]
    power, beam = pl.pallas_call(
        functools.partial(main_kernel, nelem, nchan),
        in_specs=[pl.BlockSpec(memory_space=pltpu.HBM)] * 6,
        out_specs=[pl.BlockSpec(memory_space=pltpu.VMEM)] * 2,
        out_shape=[pltpu.VMEM(o.shape, o.dtype) for o in out_shape],
        scratch_shapes=[
            pltpu.SMEM(delays.shape, jnp.int32),
            pltpu.SMEM(subband_map.shape, jnp.int32),
            pltpu.VMEM((chunks, rows, samples), jnp.bfloat16),
            pltpu.VMEM((taps, chan), jnp.bfloat16),
            pltpu.VMEM(beam_weights.shape, jnp.bfloat16),
            pltpu.VMEM(basis.shape, jnp.bfloat16),
            pltpu.VMEM((rows // 8, 8, window), jnp.float32),
            pltpu.VMEM((taps, 8, chan), jnp.float32),
            pltpu.VMEM((parts, FRAMES, elems, chan), jnp.bfloat16),
            pltpu.VMEM((beams * 2 * block, total), jnp.bfloat16),
            pltpu.VMEM((nchan, 2 * block, FRAMES * elems), jnp.bfloat16),
            pltpu.VMEM((count, 2 * block, FRAMES * elems), jnp.bfloat16),
            pltpu.VMEM((2 * block * FRAMES, total), jnp.bfloat16),
            pltpu.SemaphoreType.DMA((5,)),
            pltpu.SemaphoreType.DMA((chunks,)),
            pltpu.SemaphoreType.DMA,
            pltpu.SemaphoreType.DMA,
        ],
        compiler_params=pltpu.CompilerParams(
            collective_id=0, has_side_effects=True, vmem_limit_bytes=66_400_000
        ),
    )(delays, subband_map, voltages, prototype, beam_weights, basis)
    return pl.pallas_call(
        deliver_kernel,
        in_specs=[pl.BlockSpec(memory_space=pl.ANY)] * 2,
        out_specs=[pl.BlockSpec(memory_space=pl.ANY)] * 2,
        out_shape=out_shape,
        scratch_shapes=[pltpu.SemaphoreType.DMA((2,))],
        compiler_params=pltpu.CompilerParams(vmem_limit_bytes=2**20),
    )(power, beam)


def solution(mesh):
    return jax.shard_map(
        functools.partial(on_device, mesh.shape["elem"], mesh.shape["chan"]),
        mesh=mesh,
        in_specs=(
            P(None, ("elem", "chan"), None),
            P(("elem", "chan")),
            P(),
            P(),
            P("elem", None, "chan", None),
        ),
        out_specs=(P(("elem", "chan"), None), P(None, "chan", "elem")),
        check_vma=False,
    )
```

```python
import functools
import math

import jax
import jax.numpy as jnp
import numpy as np
from jax import lax
from jax.experimental import pallas as pl
from jax.experimental.pallas import tpu as pltpu
from jax.sharding import PartitionSpec as P

FRAMES = 4
LANES = 128
RADIX = 8
LOGICAL = pl.DeviceIdType.LOGICAL


def cosine(turns, chan):
    y = jnp.abs((turns & (chan - 1)) - chan // 2) - chan // 4
    x = y.astype(jnp.float32) * (2.0 * math.pi / chan)
    s = x * x
    poly = 1.0 / 362880 - s * (1.0 / 39916800)
    poly = -1.0 / 5040 + s * poly
    poly = 1.0 / 120 + s * poly
    poly = -1.0 / 6 + s * poly
    return (x + x * s * poly) * (chan**-0.5)


def split(value):
    high = value.astype(jnp.bfloat16)
    return high, (value - high.astype(jnp.float32)).astype(jnp.bfloat16)


NT = (((1,), (1,)), ((), ()))


def eight_points(x):
    def add(a, b):
        return (a[0] + b[0], a[1] + b[1])

    def sub(a, b):
        return (a[0] - b[0], a[1] - b[1])

    def minus_i(a):
        return (a[1], -a[0])

    def four(v):
        a, b = add(v[0], v[2]), sub(v[0], v[2])
        c, d = add(v[1], v[3]), minus_i(sub(v[1], v[3]))
        return [add(a, c), add(b, d), sub(a, c), sub(b, d)]

    root = math.sqrt(0.5)
    even = four([add(x[a], x[a + 4]) for a in range(4)])
    d = [sub(x[a], x[a + 4]) for a in range(4)]
    d1 = ((d[1][0] + d[1][1]) * root, (d[1][1] - d[1][0]) * root)
    d3 = ((d[3][1] - d[3][0]) * root, (-d[3][0] - d[3][1]) * root)
    odd = four([d[0], d1, minus_i(d[2]), d3])
    out = []
    for e, o in zip(even, odd):
        out += [e, o]
    return out


def turn_plan(chunk, groups, rows, delay_ref):
    lane = lax.broadcasted_iota(jnp.int32, (rows, LANES), 1)
    sub = lax.broadcasted_iota(jnp.int32, (rows, LANES), 0)
    shift = jnp.zeros((rows, LANES), jnp.int32)
    for i in range(rows):
        shift = jnp.where(sub == i, delay_ref[chunk % groups * rows + i], shift)
    return (lane + shift) & (LANES - 1), lane < LANES - shift


def turn_columns(chunk, first, last, held, plan, volt_ref, seg_ref):
    index, keep = plan

    def turned(c):
        value = volt_ref[chunk, :, pl.ds(c * LANES, LANES)].astype(jnp.float32)
        return jnp.take_along_axis(value, index, axis=1, mode="promise_in_bounds")

    now = turned(first) if held is None else held
    for c in range(first, last):
        nxt = turned(c + 1)
        seg_ref[chunk % 2, :, pl.ds(c * LANES, LANES)] = jnp.where(keep, now, nxt)
        now = nxt
    return now


def filter_column(chunk, groups, j, coef_ref, seg_ref, wave_ref):
    rows = seg_ref.shape[1]
    taps, _, chan = coef_ref.shape
    per = chan // LANES
    part, group = chunk // groups, chunk % groups
    held = [
        seg_ref[chunk % 2, :, pl.ds((b * per + j) * LANES, LANES)]
        for b in range(FRAMES + taps - 1)
    ]
    sums = [None] * FRAMES
    for t in range(taps):
        coef = coef_ref[t, :, pl.ds(j * LANES, LANES)]
        for f in range(FRAMES):
            term = coef * held[f + t]
            sums[f] = term if t == 0 else sums[f] + term
    for f in range(FRAMES):
        wave_ref[part, f, pl.ds(group * rows, rows), pl.ds(j * LANES, LANES)] = sums[f].astype(
            jnp.bfloat16
        )


def main_kernel(
    nelem,
    nchan,
    delay_hbm,
    map_hbm,
    volt_hbm,
    proto_hbm,
    weight_hbm,
    basis_hbm,
    power_ref,
    beam_ref,
    delay_ref,
    map_ref,
    volt_ref,
    proto_ref,
    raw_ref,
    basis_ref,
    seg_ref,
    coef_ref,
    wave_ref,
    weight_ref,
    send_ref,
    recv_ref,
    picked_ref,
    local_sem,
    volt_sem,
    send_sem,
    recv_sem,
):
    parts, frames, elems, chan = wave_ref.shape
    chunks, chunk_rows, _ = volt_ref.shape
    groups = chunks // parts
    taps = proto_ref.shape[0]
    count = nelem * nchan
    elem_at, chan_at = lax.axis_index("elem"), lax.axis_index("chan")
    me = elem_at * nchan + chan_at
    barrier = pltpu.get_barrier_semaphore()

    def each_partner(act):
        near_start = elem_at < nelem // 2

        def row(k, carry):
            first = jnp.where(near_start, nelem - 1 - k, k) * nchan
            for c in range(nchan):

                @pl.when(first + c != me)
                def _():
                    act(first + c, c)

            return carry

        if count <= 64:
            for k in range(nelem):
                row(k, 0)
        else:
            lax.fori_loop(0, nelem, row, 0)

    map_copy = pltpu.make_async_copy(map_hbm, map_ref, local_sem.at[0])
    proto_copy = pltpu.make_async_copy(proto_hbm, proto_ref, local_sem.at[1])
    delay_copy = pltpu.make_async_copy(delay_hbm, delay_ref, local_sem.at[2])
    basis_copy = pltpu.make_async_copy(basis_hbm, basis_ref, local_sem.at[3])
    weight_copy = pltpu.make_async_copy(weight_hbm, raw_ref, local_sem.at[4])
    volt_copies = [
        pltpu.make_async_copy(
            volt_hbm.at[k // groups, pl.ds(k % groups * chunk_rows, chunk_rows)],
            volt_ref.at[k],
            volt_sem.at[k],
        )
        for k in range(chunks)
    ]
    map_copy.start()
    proto_copy.start()
    delay_copy.start()
    ahead = min(4, chunks)
    for copy in volt_copies[:ahead]:
        copy.start()

    def greet(other, c):
        pl.semaphore_signal(barrier, inc=1, device_id=other, device_id_type=LOGICAL)

    each_partner(greet)
    map_copy.wait()

    subbands = map_ref.shape[0]
    block = subbands // nchan
    rows = 2 * subbands
    row = lax.broadcasted_iota(jnp.int32, (rows, LANES), 0)
    band = (row // (2 * block)) * block + row % block
    wanted = jnp.zeros((rows, LANES), jnp.int32)
    for s in range(subbands):
        wanted = jnp.where(band == s, map_ref[s], wanted)
    quarter = ((row // block) % 2) * (chan // 4)
    lane = lax.broadcasted_iota(jnp.int32, (rows, LANES), 1)
    real_basis, imag_basis = [], []
    for j in range(chan // LANES):
        turns = wanted * (lane + j * LANES) + quarter
        real_basis.append(cosine(turns, chan))
        imag_basis.append(cosine(turns + 3 * (chan // 4), chan))
    real_basis = split(jnp.concatenate(real_basis, axis=1))
    imag_basis = split(jnp.concatenate(imag_basis, axis=1))
    proto_copy.wait()
    for t in range(taps):
        coef_ref[t] = jnp.broadcast_to(
            proto_ref[pl.ds(t, 1), :].astype(jnp.float32), (8, chan)
        )
    delay_copy.wait()

    per = chan // LANES
    step = (frames + taps - 1) * per // per

    def arrive(k):
        volt_copies[k].wait()
        if k + ahead < chunks:
            volt_copies[k + ahead].start()
        elif k + ahead == chunks:
            basis_copy.start()
            weight_copy.start()

    arrive(0)
    plan = turn_plan(0, groups, chunk_rows, delay_ref)
    turn_columns(0, 0, step * per, None, plan, volt_ref, seg_ref)
    for k in range(chunks):
        held = None
        if k + 1 < chunks:
            arrive(k + 1)
            plan = turn_plan(k + 1, groups, chunk_rows, delay_ref)
        for j in range(per):
            filter_column(k, groups, j, coef_ref, seg_ref, wave_ref)
            if k + 1 < chunks:
                held = turn_columns(
                    k + 1, j * step, (j + 1) * step, held, plan, volt_ref, seg_ref
                )

    wave = [wave_ref[r].reshape(frames * elems, chan) for r in range(2)]
    chosen = jnp.zeros((rows, frames * elems), jnp.float32)
    for r, basis in ((0, real_basis), (1, imag_basis)):
        for piece in basis:
            chosen = chosen + lax.dot_general(
                piece, wave[r], NT, preferred_element_type=jnp.float32
            )
    chosen = chosen.astype(jnp.bfloat16)
    for c in range(nchan):
        send_ref[c] = chosen[2 * block * c : 2 * block * (c + 1)]

    pl.semaphore_wait(barrier, count - 1)

    def send(other, c):
        pltpu.make_async_remote_copy(
            src_ref=send_ref.at[c],
            dst_ref=recv_ref.at[me],
            send_sem=send_sem,
            recv_sem=recv_sem,
            device_id=other,
            device_id_type=LOGICAL,
        ).start()

    each_partner(send)
    recv_ref[me] = send_ref[chan_at]

    lanes = chan // RADIX
    split_wave = [
        tuple(wave[r][:, a * lanes : (a + 1) * lanes].astype(jnp.float32) for r in range(2))
        for a in range(RADIX)
    ]
    classes = eight_points(split_wave)
    basis_copy.wait()
    powers = []
    for c in range(RADIX):
        mixed = jnp.concatenate(classes[c], axis=1).astype(jnp.bfloat16)
        spec = jnp.dot(mixed, basis_ref[c], preferred_element_type=jnp.float32)
        both = spec[:, :lanes] * spec[:, :lanes] + spec[:, lanes:] * spec[:, lanes:]
        total = both[:elems]
        for f in range(1, frames):
            total = total + both[f * elems : (f + 1) * elems]
        powers.append(total * (1.0 / frames))
    wide = lanes // RADIX
    at = lax.broadcasted_iota(jnp.int32, (elems, lanes), 1)
    mixed = []
    for e in range(RADIX):
        piece = None
        for c in range(RADIX):
            shift = (wide * (c - e)) % lanes
            moved = pltpu.roll(powers[c], shift, 1) if shift else powers[c]
            piece = moved if piece is None else jnp.where(at // wide == c, moved, piece)
        mixed.append(piece)
    mixed = jnp.concatenate(mixed, axis=0).astype(jnp.bfloat16)
    down = lax.broadcasted_iota(jnp.int32, (lanes, lanes), 0)
    over = lax.broadcasted_iota(jnp.int32, (lanes, lanes), 1)
    order = (over == (down % wide) * RADIX + down // wide).astype(jnp.float32)
    final = jnp.dot(mixed, order.astype(jnp.bfloat16), preferred_element_type=jnp.float32)
    for e in range(RADIX):
        power_ref[:, e * lanes : (e + 1) * lanes] = final[e * elems : (e + 1) * elems].astype(
            jnp.bfloat16
        )

    weight_rows = weight_ref.shape[0]
    beams = weight_rows // (2 * block)
    down = lax.broadcasted_iota(jnp.int32, (weight_rows, 2 * beams), 0)
    over = lax.broadcasted_iota(jnp.int32, (weight_rows, 2 * beams), 1)
    gather = (down // (2 * block) == over % beams) & ((down // block) % 2 == over // beams)
    gather = gather.astype(jnp.float32).astype(jnp.bfloat16)
    weight_copy.wait()
    step = min(8, raw_ref.shape[0])
    for i in range(0, raw_ref.shape[0], step):
        piece = raw_ref[i : i + step].reshape(step * 2 * block, raw_ref.shape[3])
        weight_ref[2 * block * i : 2 * block * (i + step)] = piece

    arrived = recv_ref.at[pl.ds(0, count - 1)]
    pltpu.make_async_copy(arrived, arrived, recv_sem).wait()

    group = LANES // elems
    inside = lax.broadcasted_iota(jnp.int32, (2 * block, LANES), 1) // elems

    def place(q, carry):
        tiles = [recv_ref[q * group + i].astype(jnp.float32) for i in range(group)]
        pieces = []
        for f in range(frames):
            piece = None
            for i in range(group):
                shift = (elems * (i - f)) % LANES
                moved = pltpu.roll(tiles[i], shift, 1) if shift else tiles[i]
                piece = moved if piece is None else jnp.where(inside == i, moved, piece)
            pieces.append(piece)
        where = pl.multiple_of(q * LANES, LANES)
        picked_ref[:, pl.ds(where, LANES)] = jnp.concatenate(pieces, axis=0).astype(jnp.bfloat16)
        return carry

    steps = count // group
    if steps <= 8:
        for q in range(steps):
            place(q, 0)
    else:
        lax.fori_loop(0, steps, place, 0)
    product = lax.dot_general(
        picked_ref[...], weight_ref[...], NT, preferred_element_type=jnp.float32
    )
    at = lax.broadcasted_iota(jnp.int32, product.shape, 1)
    row = lax.broadcasted_iota(jnp.int32, product.shape, 0)
    product = jnp.where(at % block == row % block, product, 0.0)
    high, low = split(product)
    summed = jnp.dot(high, gather, preferred_element_type=jnp.float32) + jnp.dot(
        low, gather, preferred_element_type=jnp.float32
    )
    for f in range(frames):
        top = summed[2 * block * f : 2 * block * f + block]
        bottom = summed[2 * block * f + block : 2 * block * (f + 1)]
        real = top[:, :beams] - bottom[:, beams:]
        imag = bottom[:, :beams] + top[:, beams:]
        for s in range(block):
            beam_ref[0, pl.ds(s * frames + f, 1), :] = real[s : s + 1]
            beam_ref[1, pl.ds(s * frames + f, 1), :] = imag[s : s + 1]

    pltpu.make_async_copy(arrived, arrived, send_sem).wait()


def class_basis(chan):
    lanes = chan // RADIX
    b = np.arange(lanes)[:, None]
    d = np.arange(lanes)[None, :]
    out = []
    for c in range(RADIX):
        angle = 2.0 * np.pi / chan * (b * (c + RADIX * d) % chan)
        cos, sin = np.cos(angle) * chan**-0.5, np.sin(angle) * chan**-0.5
        out.append(np.block([[cos, -sin], [sin, cos]]))
    return jnp.asarray(np.stack(out), jnp.bfloat16)


def deliver_kernel(power_from, beam_from, power_to, beam_to, sems):
    copies = [
        pltpu.make_async_copy(power_from, power_to, sems.at[0]),
        pltpu.make_async_copy(beam_from, beam_to, sems.at[1]),
    ]
    for copy in copies:
        copy.start()
    for copy in copies:
        copy.wait()


def on_device(nelem, nchan, voltages, delays, prototype, subband_map, beam_weights):
    parts, elems, samples = voltages.shape
    taps, chan = prototype.shape
    beams, _, block, total = beam_weights.shape
    window = (FRAMES + taps - 1) * chan
    basis = class_basis(chan)
    count = nelem * nchan
    rows = 8
    chunks = parts * elems // rows
    out_shape = [
        jax.ShapeDtypeStruct((elems, chan), jnp.bfloat16),
        jax.ShapeDtypeStruct((2, block * FRAMES, beams), jnp.float32),
    ]
    power, beam = pl.pallas_call(
        functools.partial(main_kernel, nelem, nchan),
        in_specs=[pl.BlockSpec(memory_space=pltpu.HBM)] * 6,
        out_specs=[pl.BlockSpec(memory_space=pltpu.VMEM)] * 2,
        out_shape=[pltpu.VMEM(o.shape, o.dtype) for o in out_shape],
        scratch_shapes=[
            pltpu.SMEM(delays.shape, jnp.int32),
            pltpu.SMEM(subband_map.shape, jnp.int32),
            pltpu.VMEM((chunks, rows, samples), jnp.bfloat16),
            pltpu.VMEM((taps, chan), jnp.bfloat16),
            pltpu.VMEM(beam_weights.shape, jnp.bfloat16),
            pltpu.VMEM(basis.shape, jnp.bfloat16),
            pltpu.VMEM((2, rows, window), jnp.float32),
            pltpu.VMEM((taps, rows, chan), jnp.float32),
            pltpu.VMEM((parts, FRAMES, elems, chan), jnp.bfloat16),
            pltpu.VMEM((beams * 2 * block, total), jnp.bfloat16),
            pltpu.VMEM((nchan, 2 * block, FRAMES * elems), jnp.bfloat16),
            pltpu.VMEM((count, 2 * block, FRAMES * elems), jnp.bfloat16),
            pltpu.VMEM((2 * block * FRAMES, total), jnp.bfloat16),
            pltpu.SemaphoreType.DMA((5,)),
            pltpu.SemaphoreType.DMA((chunks,)),
            pltpu.SemaphoreType.DMA,
            pltpu.SemaphoreType.DMA,
        ],
        compiler_params=pltpu.CompilerParams(
            collective_id=0, has_side_effects=True, vmem_limit_bytes=66_400_000
        ),
    )(delays, subband_map, voltages, prototype, beam_weights, basis)
    return pl.pallas_call(
        deliver_kernel,
        in_specs=[pl.BlockSpec(memory_space=pl.ANY)] * 2,
        out_specs=[pl.BlockSpec(memory_space=pl.ANY)] * 2,
        out_shape=out_shape,
        scratch_shapes=[pltpu.SemaphoreType.DMA((2,))],
        compiler_params=pltpu.CompilerParams(vmem_limit_bytes=2**20),
    )(power, beam)


def solution(mesh):
    return jax.shard_map(
        functools.partial(on_device, mesh.shape["elem"], mesh.shape["chan"]),
        mesh=mesh,
        in_specs=(
            P(None, ("elem", "chan"), None),
            P(("elem", "chan")),
            P(),
            P(),
            P("elem", None, "chan", None),
        ),
        out_specs=(P(("elem", "chan"), None), P(None, "chan", "elem")),
        check_vma=False,
    )
```

```python
import functools
import math

import jax
import jax.numpy as jnp
import numpy as np
from jax import lax
from jax.experimental import pallas as pl
from jax.experimental.pallas import tpu as pltpu
from jax.sharding import PartitionSpec as P

FRAMES = 4
LANES = 128
RADIX = 8
LOGICAL = pl.DeviceIdType.LOGICAL


def cosine(turns, chan):
    y = jnp.abs((turns & (chan - 1)) - chan // 2) - chan // 4
    x = y.astype(jnp.float32) * (2.0 * math.pi / chan)
    s = x * x
    poly = 1.0 / 362880 - s * (1.0 / 39916800)
    poly = -1.0 / 5040 + s * poly
    poly = 1.0 / 120 + s * poly
    poly = -1.0 / 6 + s * poly
    return (x + x * s * poly) * (chan**-0.5)


def split(value):
    high = value.astype(jnp.bfloat16)
    return high, (value - high.astype(jnp.float32)).astype(jnp.bfloat16)


NT = (((1,), (1,)), ((), ()))


def eight_points(x):
    def add(a, b):
        return (a[0] + b[0], a[1] + b[1])

    def sub(a, b):
        return (a[0] - b[0], a[1] - b[1])

    def minus_i(a):
        return (a[1], -a[0])

    def four(v):
        a, b = add(v[0], v[2]), sub(v[0], v[2])
        c, d = add(v[1], v[3]), minus_i(sub(v[1], v[3]))
        return [add(a, c), add(b, d), sub(a, c), sub(b, d)]

    root = math.sqrt(0.5)
    even = four([add(x[a], x[a + 4]) for a in range(4)])
    d = [sub(x[a], x[a + 4]) for a in range(4)]
    d1 = ((d[1][0] + d[1][1]) * root, (d[1][1] - d[1][0]) * root)
    d3 = ((d[3][1] - d[3][0]) * root, (-d[3][0] - d[3][1]) * root)
    odd = four([d[0], d1, minus_i(d[2]), d3])
    out = []
    for e, o in zip(even, odd):
        out += [e, o]
    return out


def turn_plan(chunk, groups, rows, delay_ref):
    lane = lax.broadcasted_iota(jnp.int32, (rows, LANES), 1)
    sub = lax.broadcasted_iota(jnp.int32, (rows, LANES), 0)
    shift = jnp.zeros((rows, LANES), jnp.int32)
    for i in range(rows):
        shift = jnp.where(sub == i, delay_ref[chunk % groups * rows + i], shift)
    return (lane + shift) & (LANES - 1), lane < LANES - shift


def turn_columns(chunk, first, last, held, plan, volt_ref, seg_ref):
    index, keep = plan

    def turned(c):
        value = volt_ref[chunk, :, pl.ds(c * LANES, LANES)].astype(jnp.float32)
        return jnp.take_along_axis(value, index, axis=1, mode="promise_in_bounds")

    now = turned(first) if held is None else held
    for c in range(first, last):
        nxt = turned(c + 1)
        seg_ref[chunk % 2, :, pl.ds(c * LANES, LANES)] = jnp.where(keep, now, nxt)
        now = nxt
    return now


def filter_column(chunk, groups, j, coef_ref, seg_ref, wave_ref):
    rows = seg_ref.shape[1]
    taps, _, chan = coef_ref.shape
    per = chan // LANES
    part, group = chunk // groups, chunk % groups
    held = [
        seg_ref[chunk % 2, :, pl.ds((b * per + j) * LANES, LANES)]
        for b in range(FRAMES + taps - 1)
    ]
    sums = [None] * FRAMES
    for t in range(taps):
        coef = coef_ref[t, :, pl.ds(j * LANES, LANES)]
        for f in range(FRAMES):
            term = coef * held[f + t]
            sums[f] = term if t == 0 else sums[f] + term
    for f in range(FRAMES):
        wave_ref[part, f, pl.ds(group * rows, rows), pl.ds(j * LANES, LANES)] = sums[f].astype(
            jnp.bfloat16
        )


def main_kernel(
    nelem,
    nchan,
    delay_hbm,
    map_hbm,
    volt_hbm,
    proto_hbm,
    weight_hbm,
    basis_hbm,
    power_ref,
    beam_ref,
    delay_ref,
    map_ref,
    volt_ref,
    proto_ref,
    raw_ref,
    basis_ref,
    seg_ref,
    coef_ref,
    wave_ref,
    weight_ref,
    send_ref,
    recv_ref,
    picked_ref,
    local_sem,
    volt_sem,
    send_sem,
    recv_sem,
):
    parts, frames, elems, chan = wave_ref.shape
    chunks, chunk_rows, _ = volt_ref.shape
    groups = chunks // parts
    taps = proto_ref.shape[0]
    count = nelem * nchan
    elem_at, chan_at = lax.axis_index("elem"), lax.axis_index("chan")
    me = elem_at * nchan + chan_at
    barrier = pltpu.get_barrier_semaphore()

    def each_partner(act):
        near_start = elem_at < nelem // 2

        def row(k, carry):
            first = jnp.where(near_start, nelem - 1 - k, k) * nchan
            for c in range(nchan):

                @pl.when(first + c != me)
                def _():
                    act(first + c, c)

            return carry

        if count <= 64:
            for k in range(nelem):
                row(k, 0)
        else:
            lax.fori_loop(0, nelem, row, 0)

    map_copy = pltpu.make_async_copy(map_hbm, map_ref, local_sem.at[0])
    proto_copy = pltpu.make_async_copy(proto_hbm, proto_ref, local_sem.at[1])
    delay_copy = pltpu.make_async_copy(delay_hbm, delay_ref, local_sem.at[2])
    basis_copy = pltpu.make_async_copy(basis_hbm, basis_ref, local_sem.at[3])
    weight_copy = pltpu.make_async_copy(weight_hbm, raw_ref, local_sem.at[4])
    volt_copies = [
        pltpu.make_async_copy(
            volt_hbm.at[k // groups, pl.ds(k % groups * chunk_rows, chunk_rows)],
            volt_ref.at[k],
            volt_sem.at[k],
        )
        for k in range(chunks)
    ]
    map_copy.start()
    proto_copy.start()
    delay_copy.start()
    ahead = min(4, chunks)
    for copy in volt_copies[:ahead]:
        copy.start()

    def greet(other, c):
        pl.semaphore_signal(barrier, inc=1, device_id=other, device_id_type=LOGICAL)

    each_partner(greet)
    map_copy.wait()

    subbands = map_ref.shape[0]
    block = subbands // nchan
    rows = 2 * subbands
    row = lax.broadcasted_iota(jnp.int32, (rows, LANES), 0)
    band = (row // (2 * block)) * block + row % block
    wanted = jnp.zeros((rows, LANES), jnp.int32)
    for s in range(subbands):
        wanted = jnp.where(band == s, map_ref[s], wanted)
    quarter = ((row // block) % 2) * (chan // 4)
    lane = lax.broadcasted_iota(jnp.int32, (rows, LANES), 1)
    real_basis, imag_basis = [], []
    for j in range(chan // LANES):
        turns = wanted * (lane + j * LANES) + quarter
        real_basis.append(cosine(turns, chan))
        imag_basis.append(cosine(turns + 3 * (chan // 4), chan))
    real_basis = jnp.concatenate(split(jnp.concatenate(real_basis, axis=1)), axis=0)
    imag_basis = jnp.concatenate(split(jnp.concatenate(imag_basis, axis=1)), axis=0)
    proto_copy.wait()
    for t in range(taps):
        coef_ref[t] = jnp.broadcast_to(
            proto_ref[pl.ds(t, 1), :].astype(jnp.float32), (8, chan)
        )
    delay_copy.wait()

    per = chan // LANES
    step = (frames + taps - 1) * per // per

    def arrive(k):
        volt_copies[k].wait()
        if k + ahead < chunks:
            volt_copies[k + ahead].start()
        elif k + ahead == chunks:
            basis_copy.start()
            weight_copy.start()

    def pick(r, basis):
        return lax.dot_general(
            basis,
            wave_ref[r].reshape(frames * elems, chan),
            NT,
            preferred_element_type=jnp.float32,
        )

    arrive(0)
    plan = turn_plan(0, groups, chunk_rows, delay_ref)
    turn_columns(0, 0, step * per, None, plan, volt_ref, seg_ref)
    for k in range(chunks):
        held = None
        if k + 1 < chunks:
            arrive(k + 1)
            plan = turn_plan(k + 1, groups, chunk_rows, delay_ref)
        if k == groups:
            both = pick(0, real_basis)
        for j in range(per):
            filter_column(k, groups, j, coef_ref, seg_ref, wave_ref)
            if k + 1 < chunks:
                held = turn_columns(
                    k + 1, j * step, (j + 1) * step, held, plan, volt_ref, seg_ref
                )

    wave = [wave_ref[r].reshape(frames * elems, chan) for r in range(2)]
    both = both + pick(1, imag_basis)
    chosen = (both[:rows] + both[rows:]).astype(jnp.bfloat16)
    for c in range(nchan):
        send_ref[c] = chosen[2 * block * c : 2 * block * (c + 1)]

    pl.semaphore_wait(barrier, count - 1)

    def send(other, c):
        pltpu.make_async_remote_copy(
            src_ref=send_ref.at[c],
            dst_ref=recv_ref.at[me],
            send_sem=send_sem,
            recv_sem=recv_sem,
            device_id=other,
            device_id_type=LOGICAL,
        ).start()

    each_partner(send)
    recv_ref[me] = send_ref[chan_at]

    lanes = chan // RADIX
    split_wave = [
        tuple(wave[r][:, a * lanes : (a + 1) * lanes].astype(jnp.float32) for r in range(2))
        for a in range(RADIX)
    ]
    classes = eight_points(split_wave)
    basis_copy.wait()
    powers = []
    for c in range(RADIX):
        mixed = jnp.concatenate(classes[c], axis=1).astype(jnp.bfloat16)
        spec = jnp.dot(mixed, basis_ref[c], preferred_element_type=jnp.float32)
        both = spec[:, :lanes] * spec[:, :lanes] + spec[:, lanes:] * spec[:, lanes:]
        total = both[:elems]
        for f in range(1, frames):
            total = total + both[f * elems : (f + 1) * elems]
        powers.append(total * (1.0 / frames))
    wide = lanes // RADIX
    at = lax.broadcasted_iota(jnp.int32, (elems, lanes), 1)
    mixed = []
    for e in range(RADIX):
        piece = None
        for c in range(RADIX):
            shift = (wide * (c - e)) % lanes
            moved = pltpu.roll(powers[c], shift, 1) if shift else powers[c]
            piece = moved if piece is None else jnp.where(at // wide == c, moved, piece)
        mixed.append(piece)
    mixed = jnp.concatenate(mixed, axis=0).astype(jnp.bfloat16)
    down = lax.broadcasted_iota(jnp.int32, (lanes, lanes), 0)
    over = lax.broadcasted_iota(jnp.int32, (lanes, lanes), 1)
    order = (over == (down % wide) * RADIX + down // wide).astype(jnp.float32)
    final = jnp.dot(mixed, order.astype(jnp.bfloat16), preferred_element_type=jnp.float32)
    for e in range(RADIX):
        power_ref[:, e * lanes : (e + 1) * lanes] = final[e * elems : (e + 1) * elems].astype(
            jnp.bfloat16
        )

    weight_rows = weight_ref.shape[0]
    beams = weight_rows // (2 * block)
    down = lax.broadcasted_iota(jnp.int32, (weight_rows, 2 * beams), 0)
    over = lax.broadcasted_iota(jnp.int32, (weight_rows, 2 * beams), 1)
    gather = (down // (2 * block) == over % beams) & ((down // block) % 2 == over // beams)
    gather = gather.astype(jnp.float32).astype(jnp.bfloat16)
    weight_copy.wait()
    step = min(8, raw_ref.shape[0])
    for i in range(0, raw_ref.shape[0], step):
        piece = raw_ref[i : i + step].reshape(step * 2 * block, raw_ref.shape[3])
        weight_ref[2 * block * i : 2 * block * (i + step)] = piece

    arrived = recv_ref.at[pl.ds(0, count - 1)]
    pltpu.make_async_copy(arrived, arrived, recv_sem).wait()

    group = LANES // elems
    inside = lax.broadcasted_iota(jnp.int32, (2 * block, LANES), 1) // elems

    def place(q, carry):
        tiles = [recv_ref[q * group + i].astype(jnp.float32) for i in range(group)]
        pieces = []
        for f in range(frames):
            piece = None
            for i in range(group):
                shift = (elems * (i - f)) % LANES
                moved = pltpu.roll(tiles[i], shift, 1) if shift else tiles[i]
                piece = moved if piece is None else jnp.where(inside == i, moved, piece)
            pieces.append(piece)
        where = pl.multiple_of(q * LANES, LANES)
        picked_ref[:, pl.ds(where, LANES)] = jnp.concatenate(pieces, axis=0).astype(jnp.bfloat16)
        return carry

    steps = count // group
    if steps <= 8:
        for q in range(steps):
            place(q, 0)
    else:
        lax.fori_loop(0, steps, place, 0)
    product = lax.dot_general(
        picked_ref[...], weight_ref[...], NT, preferred_element_type=jnp.float32
    )
    at = lax.broadcasted_iota(jnp.int32, product.shape, 1)
    row = lax.broadcasted_iota(jnp.int32, product.shape, 0)
    product = jnp.where(at % block == row % block, product, 0.0)
    high, low = split(product)
    summed = jnp.dot(high, gather, preferred_element_type=jnp.float32) + jnp.dot(
        low, gather, preferred_element_type=jnp.float32
    )
    for f in range(frames):
        top = summed[2 * block * f : 2 * block * f + block]
        bottom = summed[2 * block * f + block : 2 * block * (f + 1)]
        real = top[:, :beams] - bottom[:, beams:]
        imag = bottom[:, :beams] + top[:, beams:]
        for s in range(block):
            beam_ref[0, pl.ds(s * frames + f, 1), :] = real[s : s + 1]
            beam_ref[1, pl.ds(s * frames + f, 1), :] = imag[s : s + 1]

    pltpu.make_async_copy(arrived, arrived, send_sem).wait()


def class_basis(chan):
    lanes = chan // RADIX
    b = np.arange(lanes)[:, None]
    d = np.arange(lanes)[None, :]
    out = []
    for c in range(RADIX):
        angle = 2.0 * np.pi / chan * (b * (c + RADIX * d) % chan)
        cos, sin = np.cos(angle) * chan**-0.5, np.sin(angle) * chan**-0.5
        out.append(np.block([[cos, -sin], [sin, cos]]))
    return jnp.asarray(np.stack(out), jnp.bfloat16)


def deliver_kernel(power_from, beam_from, power_to, beam_to, sems):
    copies = [
        pltpu.make_async_copy(power_from, power_to, sems.at[0]),
        pltpu.make_async_copy(beam_from, beam_to, sems.at[1]),
    ]
    for copy in copies:
        copy.start()
    for copy in copies:
        copy.wait()


def on_device(nelem, nchan, voltages, delays, prototype, subband_map, beam_weights):
    parts, elems, samples = voltages.shape
    taps, chan = prototype.shape
    beams, _, block, total = beam_weights.shape
    window = (FRAMES + taps - 1) * chan
    basis = class_basis(chan)
    count = nelem * nchan
    rows = 8
    chunks = parts * elems // rows
    out_shape = [
        jax.ShapeDtypeStruct((elems, chan), jnp.bfloat16),
        jax.ShapeDtypeStruct((2, block * FRAMES, beams), jnp.float32),
    ]
    power, beam = pl.pallas_call(
        functools.partial(main_kernel, nelem, nchan),
        in_specs=[pl.BlockSpec(memory_space=pltpu.HBM)] * 6,
        out_specs=[pl.BlockSpec(memory_space=pltpu.VMEM)] * 2,
        out_shape=[pltpu.VMEM(o.shape, o.dtype) for o in out_shape],
        scratch_shapes=[
            pltpu.SMEM(delays.shape, jnp.int32),
            pltpu.SMEM(subband_map.shape, jnp.int32),
            pltpu.VMEM((chunks, rows, samples), jnp.bfloat16),
            pltpu.VMEM((taps, chan), jnp.bfloat16),
            pltpu.VMEM(beam_weights.shape, jnp.bfloat16),
            pltpu.VMEM(basis.shape, jnp.bfloat16),
            pltpu.VMEM((2, rows, window), jnp.float32),
            pltpu.VMEM((taps, rows, chan), jnp.float32),
            pltpu.VMEM((parts, FRAMES, elems, chan), jnp.bfloat16),
            pltpu.VMEM((beams * 2 * block, total), jnp.bfloat16),
            pltpu.VMEM((nchan, 2 * block, FRAMES * elems), jnp.bfloat16),
            pltpu.VMEM((count, 2 * block, FRAMES * elems), jnp.bfloat16),
            pltpu.VMEM((2 * block * FRAMES, total), jnp.bfloat16),
            pltpu.SemaphoreType.DMA((5,)),
            pltpu.SemaphoreType.DMA((chunks,)),
            pltpu.SemaphoreType.DMA,
            pltpu.SemaphoreType.DMA,
        ],
        compiler_params=pltpu.CompilerParams(
            collective_id=0, has_side_effects=True, vmem_limit_bytes=66_400_000
        ),
    )(delays, subband_map, voltages, prototype, beam_weights, basis)
    return pl.pallas_call(
        deliver_kernel,
        in_specs=[pl.BlockSpec(memory_space=pl.ANY)] * 2,
        out_specs=[pl.BlockSpec(memory_space=pl.ANY)] * 2,
        out_shape=out_shape,
        scratch_shapes=[pltpu.SemaphoreType.DMA((2,))],
        compiler_params=pltpu.CompilerParams(vmem_limit_bytes=2**20),
    )(power, beam)


def solution(mesh):
    return jax.shard_map(
        functools.partial(on_device, mesh.shape["elem"], mesh.shape["chan"]),
        mesh=mesh,
        in_specs=(
            P(None, ("elem", "chan"), None),
            P(("elem", "chan")),
            P(),
            P(),
            P("elem", None, "chan", None),
        ),
        out_specs=(P(("elem", "chan"), None), P(None, "chan", "elem")),
        check_vma=False,
    )
```
